32 devices in a mesh: seq: 32 (over z, y, x, core).
Axes of the slice: x: 2, y: 2, z: 4, core: 2. Of those that a mesh axis runs over, the one named last changes fastest.
Arguments:
- inputs: bfloat16 [4096, 4096], P('seq'), may hold values from -6 to 6
- step_sizes: bfloat16 [4096, 4096], P('seq'), may hold values from 0.25 to 2
- cotangent: bfloat16 [4096, 4096], P('seq'), may hold values from -6 to 6
- input_coeffs: float32 [16, 4096], P(None, 'seq'), may hold values from -0.3 to 0.3
- output_coeffs: float32 [16, 4096], P(None, 'seq'), may hold values from -0.3 to 0.3
- decay_rates: float32 [16, 4096], replicated, as said below
Outputs:
- grad_inputs: bfloat16 [4096, 4096], P('seq')
- grad_steps: bfloat16 [4096, 4096], P('seq')
- grad_in_coeffs: float32 [16, 4096], P(None, 'seq')
- grad_out_coeffs: float32 [16, 4096], P(None, 'seq')
- grad_rates: float32 [16, 4096], P(None, 'seq')
The draws below stay inside these ranges and needn't reach their ends.
Inputs may be any that keep to these rules, and one draw needn't show every extreme that they name: `decay_rates`: every entry lies between 0.1 / 4096 and 0.15.
All inputs are finite; a program needn't handle non-finite values.
Results may differ from the reference program's by a relative error of at most 0.001.
Values sent between devices are 32-bit elements; how exact they have to be, the bound alone decides.
A program may use at most 64 MiB of HBM per device.

```python
import math
from functools import partial
import jax
import jax.numpy as jnp
from jax import lax

CHANNELS = 4096
STATE = 16
TOK_DEV = 128
TOKENS = 4096


def draw_decay_rates(key, part):
    chooser_key, slow_key, fast_key = jax.random.split(jax.random.fold_in(key, 7), 3)
    chooser = jax.random.uniform(chooser_key, (CHANNELS,), jnp.float32)
    fast_rates = jnp.exp(jax.random.uniform(fast_key, (STATE, CHANNELS), jnp.float32, math.log(0.05), math.log(0.15)))
    slow_share = 0.5
    slow_rates = jnp.exp(jax.random.uniform(slow_key, (STATE, CHANNELS), jnp.float32, math.log(0.3), 0.0)) / TOK_DEV
    return jnp.where(chooser[None, :] < slow_share, slow_rates, fast_rates).astype(jnp.float32)


def draw_step_sizes(key, part):
    level_key, jitter_key = jax.random.split(jax.random.fold_in(key, 11), 2)
    run_count = TOKENS // 128
    levels = jax.random.uniform(level_key, (run_count, 1, CHANNELS), jnp.float32, -0.6, 1.2)
    jitter = jax.random.uniform(jitter_key, (run_count, 128, CHANNELS), jnp.float32, -0.5, 0.5)
    values = jnp.clip(0.5 * jnp.exp(levels + jitter), 0.25, 2.0)
    return values.reshape(TOKENS, CHANNELS).astype(jnp.bfloat16)


def block_levels(rng, shape, cuts, least, top_value):
    loudness, own = 1.0, jax.random.fold_in(rng, 6)
    for axis_at, shards_of in cuts:
        heights = jnp.exp(jax.random.uniform(jax.random.fold_in(own, axis_at), (shards_of,), jnp.float32, least / len(cuts), top_value / len(cuts)))
        loudness = loudness * jnp.repeat(heights, shape[axis_at] // shards_of).reshape([-1 if axis == axis_at else 1 for axis in range(len(shape))])
    return loudness


def scatter_about(rng, extent, deviation, reach, cuts=(), dtype=jnp.bfloat16):
    entries = deviation * jax.random.normal(rng, extent, jnp.float32)
    if cuts:
        entries = entries * block_levels(rng, extent, cuts, -0.22, 0.18)
    return jnp.clip(entries, -reach, reach).astype(dtype)


def setup_inputs(seed: int = 0) -> dict:
    key_list = jax.random.split(jax.random.key(seed), 7)
    inputs = scatter_about(key_list[0], (TOKENS, CHANNELS), 1.0, 6.0, ((0, 32),))
    step_sizes = draw_step_sizes(jax.random.fold_in(key_list[6], 71), 0)
    cotangent = scatter_about(key_list[2], (TOKENS, CHANNELS), 1.0, 6.0, ((0, 32),))
    input_coeffs = scatter_about(key_list[3], (STATE, TOKENS), 0.05, 0.3, ((1, 32),), jnp.float32)
    output_coeffs = scatter_about(key_list[4], (STATE, TOKENS), 0.05, 0.3, ((1, 32),), jnp.float32)
    decay_rates = draw_decay_rates(jax.random.fold_in(key_list[6], 71), 0)
    return {"inputs": inputs, "step_sizes": step_sizes, "cotangent": cotangent, "input_coeffs": input_coeffs, "output_coeffs": output_coeffs, "decay_rates": decay_rates}


block_len = 32


def blocked(array):
    return array.reshape(array.shape[0] // block_len, block_len, array.shape[1])


def sweep_forward(initial, inputs, step_sizes, in_rows, decay_rates):
    def per_block(hidden, block_data):
        block_input, block_delta, block_bcoef = block_data
        anchor = hidden
        for position in range(block_len):
            row_delta = block_delta[position].astype(jnp.float32)
            decay_row = jnp.exp(-row_delta[None, :] * decay_rates)
            drive = block_bcoef[position][:, None] * (row_delta * block_input[position].astype(jnp.float32))[None, :]
            hidden = decay_row * hidden + drive
        return hidden, anchor
    return lax.scan(per_block, initial, (blocked(inputs), blocked(step_sizes), blocked(in_rows)))


def block_grads(carried, block_data, decay_rates):
    later, grad_rates = carried
    anchor, block_input, block_delta, block_bcoef, block_ccoef, block_grad = block_data
    hidden_list = [anchor]
    for position in range(block_len):
        row_delta = block_delta[position].astype(jnp.float32)
        decay_row = jnp.exp(-row_delta[None, :] * decay_rates)
        drive = block_bcoef[position][:, None] * (row_delta * block_input[position].astype(jnp.float32))[None, :]
        hidden_list.append(decay_row * hidden_list[-1] + drive)
    input_rows = [None] * block_len
    step_rows = [None] * block_len
    bcoef_rows = [None] * block_len
    ccoef_rows = [None] * block_len
    for position in reversed(range(block_len)):
        row_delta = block_delta[position].astype(jnp.float32)
        row_input = block_input[position].astype(jnp.float32)
        row_grad = block_grad[position].astype(jnp.float32)
        decay_row = jnp.exp(-row_delta[None, :] * decay_rates)
        grad_state = block_ccoef[position][:, None] * row_grad[None, :] + later
        coeff_sum = jnp.sum(grad_state * block_bcoef[position][:, None], 0)
        weighted = grad_state * decay_row * hidden_list[position]
        input_rows[position] = (row_delta * coeff_sum).astype(jnp.bfloat16)
        step_rows[position] = (row_input * coeff_sum - jnp.sum(weighted * decay_rates, 0)).astype(jnp.bfloat16)
        bcoef_rows[position] = jnp.sum(grad_state * (row_delta * row_input)[None, :], 1)
        ccoef_rows[position] = jnp.sum(hidden_list[position + 1] * row_grad[None, :], 1)
        grad_rates = grad_rates - weighted * row_delta[None, :]
        later = decay_row * grad_state
    return (later, grad_rates), (jnp.stack(input_rows), jnp.stack(step_rows), jnp.stack(bcoef_rows), jnp.stack(ccoef_rows))


def reference(inputs, step_sizes, cotangent, input_coeffs, output_coeffs, decay_rates):
    blank = jnp.zeros(decay_rates.shape, jnp.float32)
    in_rows = input_coeffs.T
    out_rows = output_coeffs.T
    _, anchors = sweep_forward(blank, inputs, step_sizes, in_rows, decay_rates)
    block_data = (anchors, blocked(inputs), blocked(step_sizes), blocked(in_rows), blocked(out_rows), blocked(cotangent))
    (_, grad_rates), pieces = lax.scan(partial(block_grads, decay_rates=decay_rates), (blank, blank), block_data, reverse=True)
    channels = inputs.shape[1]
    n_state = decay_rates.shape[0]
    grad_inputs = pieces[0].reshape(-1, channels)
    grad_steps = pieces[1].reshape(-1, channels)
    grad_in_coeffs = pieces[2].reshape(-1, n_state).T
    grad_out_coeffs = pieces[3].reshape(-1, n_state).T
    return (grad_inputs, grad_steps, grad_in_coeffs, grad_out_coeffs, grad_rates)
```

```python
from functools import partial
import math

import jax
import jax.numpy as jnp
from jax import lax
from jax.experimental import pallas as pl
from jax.experimental.pallas import tpu as pltpu
from jax.sharding import PartitionSpec as P

LANES = 128
SUB = 8
TILES = 4
GROUP = 8
LOG2E = math.log2(math.e)
LN2 = math.log(2.0)
F32 = jnp.float32
MESH = pl.DeviceIdType.MESH


def loop(start, stop, body):
    def step(k, _):
        body(k)
        return 0

    lax.fori_loop(start, stop, step, 0)


def expand(coef_ref, wide, tokens, n_state):
    for t in range(tokens):
        wide[t] = jnp.broadcast_to(coef_ref[:, t : t + 1], (n_state, LANES))


def lane_sums(acc, out_ref, tokens, n_state):
    lane = lax.broadcasted_iota(jnp.int32, (n_state, tokens), 1)
    total = jnp.zeros((n_state, tokens), F32)
    for t in range(tokens):
        total = jnp.where(lane == t, jnp.sum(acc[t], axis=1, keepdims=True), total)
    out_ref[...] = total


def cols(jj):
    return slice(jj * LANES, (jj + 1) * LANES)


def whole_kernel(
    n,
    x_hbm, d_hbm, g_hbm, b_hbm, c_hbm, a_hbm,
    gi_hbm, gs_hbm, gb_ref, gc_ref, gr_ref,
    xv, dv, gv, bv, cv, av, giv, gsv,
    bx, cx, accb, accc, dl, uu, gg, dec, hs, csp, awp, cs, ws, mine, own,
    sm, rv, out1, in1, out2, in2, st2, tmp, hst, rp, rr, out3, in3,
    ins, outs, d1s, d1r, i1s, i1r, i2s, i2r, d2s, d2r, d3s, d3r, i3s, i3r,
):
    me = lax.axis_index("seq")
    core, chip = lax.rem(me, 2), me // 2
    mate = 2 * chip + 1 - core
    tokens, channels = xv.shape
    n_state = av.shape[0]
    chips = n // 2
    blocks = channels // (LANES * TILES)
    pieces = blocks // 2
    share = chips // TILES
    r = n_state // share
    width = channels // n
    per = LANES // width
    first = core == 0
    barrier = pltpu.get_barrier_semaphore()

    loads = [
        pltpu.make_async_copy(src, dst, ins.at[k])
        for k, (src, dst) in enumerate(
            [(b_hbm, bv), (c_hbm, cv), (d_hbm, dv), (x_hbm, xv), (g_hbm, gv), (a_hbm, av)]
        )
    ]
    for load in loads:
        load.start()

    def tell(k):
        pl.semaphore_signal(barrier, inc=1, device_id=(lax.rem(me + k, n),), device_id_type=MESH)

    loop(1, n, tell)

    def tile_of(b, jj):
        return blocks * jj + lax.rem(b + 2 * jj, blocks)

    def lanes_of(b, jj):
        return pl.ds(pl.multiple_of(tile_of(b, jj) * LANES, LANES), LANES)

    def remote(src, dst, send_sem, recv_sem, dest):
        return pltpu.make_async_remote_copy(
            src_ref=src, dst_ref=dst, send_sem=send_sem, recv_sem=recv_sem,
            device_id=(dest,), device_id_type=MESH,
        )

    def row(ref, b, t):
        return ref.at[b][:, pl.ds(t, n_state, stride=0), :]

    def rates_of(b):
        return jnp.stack([av[:, lanes_of(b, jj)] * (-LOG2E) for jj in range(TILES)])

    state_shape = (TILES, n_state, LANES)
    groups = tokens // GROUP

    def summarize(q, half):
        b = 2 * q + half
        for jj in range(TILES):
            lanes = lanes_of(b, jj)
            delta = dv[:, lanes].astype(F32)
            dl[b, jj] = delta
            uu[b, jj] = delta * xv[:, lanes].astype(F32)
            gg[b, jj] = gv[:, lanes].astype(F32)
            sm[q, half, 2 * n_state :, cols(jj)] = jnp.sum(delta, axis=0, keepdims=True)
        rates = rates_of(b)

        def ahead(i, end):
            for s in range(GROUP):
                t = i * GROUP + s
                decay = jnp.exp2(row(dl, b, t) * rates)
                dec[b, t] = decay
                end = decay * end + bx[t][None] * row(uu, b, t)
            return end

        def behind(i, back):
            for s in reversed(range(GROUP)):
                t = tokens - GROUP - i * GROUP + s
                back = dec[b, t] * (cx[t][None] * row(gg, b, t) + back)
            return back

        zero = jnp.zeros(state_shape, F32)
        end = lax.fori_loop(0, groups, ahead, zero)
        back = lax.fori_loop(0, groups, behind, zero)
        for jj in range(TILES):
            sm[q, half, :n_state, cols(jj)] = end[jj]
            sm[q, half, n_state : 2 * n_state, cols(jj)] = back[jj]

    def mate1(q):
        return remote(sm.at[q, 1 - core], rv.at[q], d1s.at[q], d1r.at[q], mate)

    def pair_of(q, jj):
        rates = av[:, lanes_of(2 * q + core, jj)] * (-LOG2E)
        kept = sm.at[q, core]
        end_m, back_m = kept[:n_state, cols(jj)], kept[n_state : 2 * n_state, cols(jj)]
        sum_m = kept[2 * n_state :, cols(jj)]
        end_t, back_t = rv[q, :n_state, cols(jj)], rv[q, n_state : 2 * n_state, cols(jj)]
        sum_t = rv[q, 2 * n_state :, cols(jj)]
        pick = lambda a, b: (jnp.where(first, a, b), jnp.where(first, b, a))
        return rates, pick(end_m, end_t), pick(back_m, back_t), pick(sum_m, sum_t)

    def chip_copy(src, dst, send_sem, recv_sem, q, there):
        return remote(
            src.at[q, there], dst.at[q, chip], send_sem.at[q], recv_sem.at[q], 2 * there + core
        )

    def chip_sends(*refs):
        def send(k):
            chip_copy(*refs, lax.rem(chip + k, chips)).start()

        loop(1, chips, send)

    def chip_all(src, dst, send_sem, recv_sem, q):
        part = pl.ds(0, chips - 1)
        return remote(src.at[q, part], dst.at[q, part], send_sem.at[q], recv_sem.at[q], mate)

    def merge(q):
        mate1(q).wait_recv()
        for jj in range(TILES):
            rates, (end0, end1), (back0, back1), (sum0, sum1) = pair_of(q, jj)
            end = jnp.exp2(rates * sum1) * end0 + end1
            back = back0 + jnp.exp2(rates * sum0) * back1
            for i in range(share):
                slot, rows = jj * share + i, slice(i * r, (i + 1) * r)
                out1[q, slot, :r] = end[rows]
                out1[q, slot, r : 2 * r] = back[rows]
                out1[q, slot, 2 * r :] = sum0 + sum1
        in1[q, chip] = out1[q, chip]
        chip_sends(out1, in1, i1s, i1r, q)

    def scan(q):
        chip_all(out1, in1, i1s, i1r, q).wait_recv()
        rates = own[q]

        def step(c, carry):
            ahead, behind = carry
            e = chips - 1 - c
            out2[q, c, :r] = ahead
            out2[q, e, r:] = behind
            ahead = jnp.exp2(rates * in1[q, c, 2 * r :]) * ahead + in1[q, c, :r]
            behind = jnp.exp2(rates * in1[q, e, 2 * r :]) * behind + in1[q, e, r : 2 * r]
            return ahead, behind

        blank = jnp.zeros((r, LANES), F32)
        lax.fori_loop(0, chips, step, (blank, blank), unroll=8)
        in2[q, chip] = out2[q, chip]
        chip_sends(out2, in2, i2s, i2r, q)

    def mate2(q):
        return remote(tmp.at[q], hst.at[q, core], d2s.at[q], d2r.at[q], mate)

    def split(q):
        chip_all(out2, in2, i2s, i2r, q).wait_recv()
        for jj in range(TILES):
            for i in range(share):
                slot, at = jj * share + i, i * r
                st2[at : at + r, cols(jj)] = in2[q, slot, :r]
                st2[n_state + at : n_state + at + r, cols(jj)] = in2[q, slot, r:]
        for jj in range(TILES):
            rates, (end0, _), (_, back1), (sum0, sum1) = pair_of(q, jj)
            head0, tail1 = st2[:n_state, cols(jj)], st2[n_state:, cols(jj)]
            head1 = jnp.exp2(rates * sum0) * head0 + end0
            tail0 = jnp.exp2(rates * sum1) * tail1 + back1
            hst[q, core, :n_state, cols(jj)] = jnp.where(first, head0, head1)
            hst[q, core, n_state:, cols(jj)] = jnp.where(first, tail0, tail1)
            tmp[q, :n_state, cols(jj)] = jnp.where(first, head1, head0)
            tmp[q, n_state:, cols(jj)] = jnp.where(first, tail1, tail0)
        mate2(q).start()

    def out_copies(b):
        return [
            pltpu.make_async_copy(v.at[:, lanes_of(b, jj)], h.at[:, lanes_of(b, jj)], outs.at[k])
            for k, (v, h) in enumerate([(giv, gi_hbm), (gsv, gs_hbm)])
            for jj in range(TILES)
        ]

    def differentiate(q, half):
        b = 2 * q + half
        rates = rates_of(b)

        def ahead(i, hidden):
            for s in range(GROUP):
                t = i * GROUP + s
                hs[t] = hidden
                hidden = dec[b, t] * hidden + bx[t][None] * row(uu, b, t)
                accc[t] += jnp.sum(row(gg, b, t) * hidden, axis=0)
            return hidden

        start = jnp.stack([hst[q, half, :n_state, cols(jj)] for jj in range(TILES)])
        lax.fori_loop(0, groups, ahead, start)

        def behind(i, carry):
            later, rate = carry
            base = tokens - GROUP - i * GROUP
            for s in reversed(range(GROUP)):
                t = base + s
                state = cx[t][None] * row(gg, b, t) + later
                later = dec[b, t] * state
                weighted = later * hs[t]
                rate = rate + weighted * row(dl, b, t)
                one, two = state * bx[t][None], weighted * rates
                fold = pl.ds(s, SUB, stride=GROUP)
                csp[:, fold, :] = sum(one[:, h : h + SUB] for h in range(0, n_state, SUB))
                awp[:, fold, :] = sum(two[:, h : h + SUB] for h in range(0, n_state, SUB))
                accb[t] += jnp.sum(state * row(uu, b, t), axis=0)
            rows = pl.ds(pl.multiple_of(base, GROUP), GROUP)
            coeff, weigh = csp[:, :GROUP], awp[:, :GROUP]
            for k in range(1, SUB):
                coeff = coeff + csp[:, k * GROUP : (k + 1) * GROUP]
                weigh = weigh + awp[:, k * GROUP : (k + 1) * GROUP]
            cs[:, rows, :] = coeff
            ws[:, rows, :] = weigh
            return later, rate

        last = jnp.stack([hst[q, half, n_state:, cols(jj)] for jj in range(TILES)])
        _, rate = lax.fori_loop(0, groups, behind, (last, jnp.zeros(state_shape, F32)))
        for jj in range(TILES):
            lanes = lanes_of(b, jj)
            giv[:, lanes] = (dl[b, jj] * cs[jj]).astype(giv.dtype)
            gsv[:, lanes] = (xv[:, lanes].astype(F32) * cs[jj] + LN2 * ws[jj]).astype(gsv.dtype)
            rp[q, half, :, cols(jj)] = -rate[jj]
        for copy in out_copies(b):
            copy.start()

    def mate3(q):
        return remote(rp.at[q, 1 - core], rr.at[q], d3s.at[q], d3r.at[q], mate)

    def owner(q, jj, s):
        return tile_of(2 * q + core, jj) * per + s

    def rate_copy(slot, dest):
        return remote(out3.at[slot], in3.at[chip], i3s.at[slot], i3r.at[chip], dest)

    def spread(q):
        mate3(q).wait_recv()
        for jj in range(TILES):
            total = rp[q, core, :, cols(jj)] + rr[q, :, cols(jj)]
            for s in range(per):
                slot, dest = (q * TILES + jj) * per + s, owner(q, jj, s)
                out3[slot] = total[:, s * width : (s + 1) * width]

                @pl.when(dest != me)
                def _():
                    rate_copy(slot, dest).start()

                @pl.when(dest == me)
                def _():
                    in3[chip] = out3[slot]

    accb[...] = jnp.zeros_like(accb)
    accc[...] = jnp.zeros_like(accc)
    loads[0].wait()
    expand(bv, bx, tokens, n_state)
    loads[1].wait()
    expand(cv, cx, tokens, n_state)
    for load in loads[2:]:
        load.wait()
    own_tile, own_row = chip // share, lax.rem(chip, share) * r
    for q in range(pieces):
        mine[q] = av[:, lanes_of(2 * q + core, own_tile)] * (-LOG2E)
        for i in range(r):
            own[q, i : i + 1] = mine.at[q][pl.ds(own_row + i, SUB, stride=0), :][:1]

    def gather(q):
        summarize(q, 1 - core)

        @pl.when(q == 0)
        def _():
            pl.semaphore_wait(barrier, n - 1)

        mate1(q).start()

        @pl.when(q >= 2)
        def _():
            scan(q - 2)

        summarize(q, core)
        merge(q)

    loop(0, pieces, gather)
    split(0)

    def finish(q):
        half = lax.rem(core + (q + pieces - 1) // pieces, 2)

        @pl.when(q >= 1)
        def _():
            mate2(q).wait_recv()

        differentiate(q, half)

        @pl.when(q == 0)
        def _():
            scan(pieces - 2)
            scan(pieces - 1)
            mate2(0).wait_recv()

        @pl.when(q >= 1)
        def _():
            mate3(q).start()

        @pl.when(q == 1)
        def _():
            spread(0)

        @pl.when(q + 1 < pieces)
        def _():
            split(q + 1)

        differentiate(q, 1 - half)

        @pl.when(q == 0)
        def _():
            mate3(0).start()

        @pl.when(q >= 1)
        def _():
            spread(q)

    loop(0, pieces, finish)
    lane_sums(accb, gb_ref, tokens, n_state)
    lane_sums(accc, gc_ref, tokens, n_state)

    my_tile = me // per
    my_row = my_tile // blocks
    my_half = lax.rem(lax.rem(my_tile, blocks) + 2 * blocks - 2 * my_row, 2)

    def landed(c):
        sender = 2 * c + my_half

        @pl.when(sender != me)
        def _():
            remote(out3.at[0], in3.at[c], i3s.at[0], i3r.at[c], mate).wait_recv()

    loop(0, chips, landed)
    gr_ref[...] = lax.fori_loop(
        0, chips, lambda c, total: total + in3[c], jnp.zeros((n_state, width), F32)
    )
    for q in range(pieces):
        for copy in (mate1(q), mate2(q), mate3(q)):
            copy.wait_send()
        chip_all(out1, in1, i1s, i1r, q).wait_send()
        chip_all(out2, in2, i2s, i2r, q).wait_send()
        for jj in range(TILES):
            for s in range(per):
                slot, dest = (q * TILES + jj) * per + s, owner(q, jj, s)

                @pl.when(dest != me)
                def _():
                    rate_copy(slot, dest).wait_send()

    for k, (v, h) in enumerate([(giv, gi_hbm), (gsv, gs_hbm)]):
        pltpu.make_async_copy(v, h, outs.at[k]).wait()


def hand_out(*refs):
    count = (len(refs) - 2) // 3
    srcs, dsts, bufs = refs[:count], refs[count : 2 * count], refs[2 * count : 3 * count]
    into, away = refs[3 * count :]
    steps = []
    for k in range(count):
        rows = srcs[k].shape[0]
        parts = 4 if rows % 64 == 0 else 1
        for p in range(parts):
            steps.append((k, pl.ds(p * (rows // parts), rows // parts)))
    moves = [
        (
            pltpu.make_async_copy(srcs[k].at[part], bufs[k].at[part], into.at[i]),
            pltpu.make_async_copy(bufs[k].at[part], dsts[k].at[part], away.at[i]),
        )
        for i, (k, part) in enumerate(steps)
    ]
    for load, _ in moves:
        load.start()
    for load, store in moves:
        load.wait()
        store.start()
    for _, store in moves:
        store.wait()


def shards(n, inputs, step_sizes, cotangent, input_coeffs, output_coeffs, decay_rates):
    n_state, channels = decay_rates.shape
    tokens = inputs.shape[0]
    width = channels // n
    per = LANES // width
    chips = n // 2
    block = TILES * LANES
    blocks = channels // block
    pieces = blocks // 2
    r = n_state * TILES // chips
    assert r * chips == n_state * TILES and per * width == LANES
    wide = pltpu.VMEM((tokens, n_state, LANES), F32)
    rows = pltpu.VMEM((blocks, TILES, tokens, LANES), F32)
    part = pltpu.VMEM((TILES, tokens, LANES), F32)
    fold = pltpu.VMEM((TILES, GROUP * SUB, LANES), F32)
    full = pltpu.VMEM((tokens, channels), jnp.bfloat16)
    small = pltpu.VMEM((n_state, tokens), F32)
    hbm = pl.BlockSpec(memory_space=pl.ANY)
    vmem = pl.BlockSpec(memory_space=pltpu.VMEM)
    sems = pltpu.SemaphoreType.DMA((pieces,))
    outs = [
        jax.ShapeDtypeStruct((tokens, channels), jnp.bfloat16),
        jax.ShapeDtypeStruct((tokens, channels), jnp.bfloat16),
        jax.ShapeDtypeStruct((n_state, tokens), F32),
        jax.ShapeDtypeStruct((n_state, tokens), F32),
        jax.ShapeDtypeStruct((n_state, width), F32),
    ]
    results = pl.pallas_call(
        partial(whole_kernel, n),
        name="whole",
        in_specs=[hbm] * 6,
        out_specs=[hbm, hbm, vmem, vmem, vmem],
        out_shape=outs,
        scratch_shapes=[
            full, full, full, small, small, pltpu.VMEM((n_state, channels), F32), full, full,
            wide, wide, wide, wide, rows, rows, rows,
            pltpu.VMEM((blocks, tokens, TILES, n_state, LANES), F32),
            pltpu.VMEM((tokens, TILES, n_state, LANES), F32),
            fold, fold, part, part,
            pltpu.VMEM((pieces, n_state, LANES), F32),
            pltpu.VMEM((pieces, r, LANES), F32),
            pltpu.VMEM((pieces, 2, 2 * n_state + 1, block), F32),
            pltpu.VMEM((pieces, 2 * n_state + 1, block), F32),
            pltpu.VMEM((pieces, chips, 2 * r + 1, LANES), F32),
            pltpu.VMEM((pieces, chips, 2 * r + 1, LANES), F32),
            pltpu.VMEM((pieces, chips, 2 * r, LANES), F32),
            pltpu.VMEM((pieces, chips, 2 * r, LANES), F32),
            pltpu.VMEM((2 * n_state, block), F32),
            pltpu.VMEM((pieces, 2 * n_state, block), F32),
            pltpu.VMEM((pieces, 2, 2 * n_state, block), F32),
            pltpu.VMEM((pieces, 2, n_state, block), F32),
            pltpu.VMEM((pieces, n_state, block), F32),
            pltpu.VMEM((pieces * TILES * per, n_state, width), F32),
            pltpu.VMEM((chips, n_state, width), F32),
            pltpu.SemaphoreType.DMA((6,)), pltpu.SemaphoreType.DMA((2,)),
            sems, sems, sems, sems, sems, sems, sems, sems, sems, sems,
            pltpu.SemaphoreType.DMA((pieces * TILES * per,)),
            pltpu.SemaphoreType.DMA((chips,)),
        ],
        compiler_params=pltpu.CompilerParams(
            collective_id=0, has_side_effects=True, vmem_limit_bytes=63 * 1024 * 1024
        ),
    )(inputs, step_sizes, cotangent, input_coeffs, output_coeffs, decay_rates)
    moves = 11
    return pl.pallas_call(
        hand_out,
        name="hand_out",
        in_specs=[hbm] * 5,
        out_specs=[hbm] * 5,
        out_shape=outs,
        scratch_shapes=[
            *[pltpu.VMEM(o.shape, o.dtype) for o in outs],
            pltpu.SemaphoreType.DMA((moves,)), pltpu.SemaphoreType.DMA((moves,)),
        ],
    )(*results)


def solution(mesh):
    placed = (P("seq", None), P("seq", None), P("seq", None), P(None, "seq"), P(None, "seq"), P())
    return jax.shard_map(
        partial(shards, mesh.shape["seq"]),
        mesh=mesh,
        in_specs=placed,
        out_specs=(P("seq", None), P("seq", None), P(None, "seq"), P(None, "seq"), P(None, "seq")),
        check_vma=False,
    )
```

```python
from functools import partial
import math

import jax
import jax.numpy as jnp
from jax import lax
from jax.experimental import pallas as pl
from jax.experimental.pallas import tpu as pltpu
from jax.sharding import PartitionSpec as P

LANES = 128
SUB = 8
TILES = 4
GROUP = 8
SPAN = 16
LOG2E = math.log2(math.e)
LN2 = math.log(2.0)
F32 = jnp.float32
MESH = pl.DeviceIdType.MESH


def loop(start, stop, body):
    def step(k, _):
        body(k)
        return 0

    lax.fori_loop(start, stop, step, 0)


def expand(coef_ref, wide, tokens, n_state):
    for t in range(tokens):
        wide[t] = jnp.broadcast_to(coef_ref[:, t : t + 1], (n_state, LANES))


def lane_sums(acc, out_ref, tokens, n_state):
    lane = lax.broadcasted_iota(jnp.int32, (n_state, tokens), 1)
    total = jnp.zeros((n_state, tokens), F32)
    for t in range(tokens):
        total = jnp.where(lane == t, jnp.sum(acc[t], axis=1, keepdims=True), total)
    out_ref[...] = total


def cols(jj):
    return slice(jj * LANES, (jj + 1) * LANES)


def whole_kernel(
    n,
    x_hbm, d_hbm, g_hbm, b_hbm, c_hbm, a_hbm,
    gi_hbm, gs_hbm, gb_ref, gc_ref, gr_ref,
    xv, dv, gv, bv, cv, av, giv, gsv,
    bx, cx, accb, accc, dl, uu, gg, dec, hs, csp, awp, cs, ws, mine, own,
    sm, rv, out1, in1, out2, in2, st2, tmp, hst, rp, rr, out3, in3,
    ins, outs, d1s, d1r, i1s, i1r, i2s, i2r, d2s, d2r, d3s, d3r, i3s, i3r,
):
    me = lax.axis_index("seq")
    core, chip = lax.rem(me, 2), me // 2
    mate = 2 * chip + 1 - core
    tokens, channels = xv.shape
    n_state = av.shape[0]
    chips = n // 2
    blocks = channels // (LANES * TILES)
    pieces = blocks // 2
    share = chips // TILES
    r = n_state // share
    width = channels // n
    per = LANES // width
    first = core == 0
    barrier = pltpu.get_barrier_semaphore()

    loads = [
        pltpu.make_async_copy(src, dst, ins.at[k])
        for k, (src, dst) in enumerate(
            [(b_hbm, bv), (c_hbm, cv), (d_hbm, dv), (x_hbm, xv), (g_hbm, gv), (a_hbm, av)]
        )
    ]
    for load in loads:
        load.start()

    def tell(k):
        pl.semaphore_signal(barrier, inc=1, device_id=(lax.rem(me + k, n),), device_id_type=MESH)

    loop(1, n, tell)

    def tile_of(b, jj):
        return blocks * jj + lax.rem(b + 2 * jj, blocks)

    def lanes_of(b, jj):
        return pl.ds(pl.multiple_of(tile_of(b, jj) * LANES, LANES), LANES)

    def remote(src, dst, send_sem, recv_sem, dest):
        return pltpu.make_async_remote_copy(
            src_ref=src, dst_ref=dst, send_sem=send_sem, recv_sem=recv_sem,
            device_id=(dest,), device_id_type=MESH,
        )

    def row(ref, b, t):
        return ref.at[b][:, pl.ds(t, n_state, stride=0), :]

    def rates_of(b):
        return jnp.stack([av[:, lanes_of(b, jj)] * (-LOG2E) for jj in range(TILES)])

    state_shape = (TILES, n_state, LANES)
    spans = tokens // SPAN

    def summarize(q, half):
        b = 2 * q + half
        for jj in range(TILES):
            lanes = lanes_of(b, jj)
            delta = dv[:, lanes].astype(F32)
            dl[b, jj] = delta
            uu[b, jj] = delta * xv[:, lanes].astype(F32)
            gg[b, jj] = gv[:, lanes].astype(F32)
            sm[q, half, 2 * n_state :, cols(jj)] = jnp.sum(delta, axis=0, keepdims=True)
        rates = rates_of(b)

        def ahead(i, end):
            for s in range(SPAN):
                t = i * SPAN + s
                decay = jnp.exp2(row(dl, b, t) * rates)
                dec[b, t] = decay
                end = decay * end + bx[t][None] * row(uu, b, t)
            return end

        def behind(i, back):
            for s in reversed(range(SPAN)):
                t = tokens - SPAN - i * SPAN + s
                back = dec[b, t] * (cx[t][None] * row(gg, b, t) + back)
            return back

        zero = jnp.zeros(state_shape, F32)
        end = lax.fori_loop(0, spans, ahead, zero)
        back = lax.fori_loop(0, spans, behind, zero)
        for jj in range(TILES):
            sm[q, half, :n_state, cols(jj)] = end[jj]
            sm[q, half, n_state : 2 * n_state, cols(jj)] = back[jj]

    def mate1(q):
        return remote(sm.at[q, 1 - core], rv.at[q], d1s.at[q], d1r.at[q], mate)

    def pair_of(q, jj):
        rates = av[:, lanes_of(2 * q + core, jj)] * (-LOG2E)
        kept = sm.at[q, core]
        end_m, back_m = kept[:n_state, cols(jj)], kept[n_state : 2 * n_state, cols(jj)]
        sum_m = kept[2 * n_state :, cols(jj)]
        end_t, back_t = rv[q, :n_state, cols(jj)], rv[q, n_state : 2 * n_state, cols(jj)]
        sum_t = rv[q, 2 * n_state :, cols(jj)]
        pick = lambda a, b: (jnp.where(first, a, b), jnp.where(first, b, a))
        return rates, pick(end_m, end_t), pick(back_m, back_t), pick(sum_m, sum_t)

    def chip_copy(src, dst, send_sem, recv_sem, q, there):
        return remote(
            src.at[q, there], dst.at[q, chip], send_sem.at[q], recv_sem.at[q], 2 * there + core
        )

    def chip_sends(*refs):
        def send(k):
            chip_copy(*refs, lax.rem(chip + k, chips)).start()

        loop(1, chips, send)

    def chip_all(src, dst, send_sem, recv_sem, q):
        part = pl.ds(0, chips - 1)
        return remote(src.at[q, part], dst.at[q, part], send_sem.at[q], recv_sem.at[q], mate)

    def merge(q):
        mate1(q).wait_recv()
        for jj in range(TILES):
            rates, (end0, end1), (back0, back1), (sum0, sum1) = pair_of(q, jj)
            end = jnp.exp2(rates * sum1) * end0 + end1
            back = back0 + jnp.exp2(rates * sum0) * back1
            for i in range(share):
                slot, rows = jj * share + i, slice(i * r, (i + 1) * r)
                out1[q, slot, :r] = end[rows]
                out1[q, slot, r : 2 * r] = back[rows]
                out1[q, slot, 2 * r :] = sum0 + sum1
        in1[q, chip] = out1[q, chip]
        chip_sends(out1, in1, i1s, i1r, q)

    def scan(q):
        chip_all(out1, in1, i1s, i1r, q).wait_recv()
        rates = own[q]

        def step(c, carry):
            ahead, behind = carry
            e = chips - 1 - c
            out2[q, c, :r] = ahead
            out2[q, e, r:] = behind
            ahead = jnp.exp2(rates * in1[q, c, 2 * r :]) * ahead + in1[q, c, :r]
            behind = jnp.exp2(rates * in1[q, e, 2 * r :]) * behind + in1[q, e, r : 2 * r]
            return ahead, behind

        blank = jnp.zeros((r, LANES), F32)
        lax.fori_loop(0, chips, step, (blank, blank), unroll=8)
        in2[q, chip] = out2[q, chip]
        chip_sends(out2, in2, i2s, i2r, q)

    def mate2(q):
        return remote(tmp.at[q], hst.at[q, core], d2s.at[q], d2r.at[q], mate)

    def split(q):
        chip_all(out2, in2, i2s, i2r, q).wait_recv()
        for jj in range(TILES):
            for i in range(share):
                slot, at = jj * share + i, i * r
                st2[at : at + r, cols(jj)] = in2[q, slot, :r]
                st2[n_state + at : n_state + at + r, cols(jj)] = in2[q, slot, r:]
        for jj in range(TILES):
            rates, (end0, _), (_, back1), (sum0, sum1) = pair_of(q, jj)
            head0, tail1 = st2[:n_state, cols(jj)], st2[n_state:, cols(jj)]
            head1 = jnp.exp2(rates * sum0) * head0 + end0
            tail0 = jnp.exp2(rates * sum1) * tail1 + back1
            hst[q, core, :n_state, cols(jj)] = jnp.where(first, head0, head1)
            hst[q, core, n_state:, cols(jj)] = jnp.where(first, tail0, tail1)
            tmp[q, :n_state, cols(jj)] = jnp.where(first, head1, head0)
            tmp[q, n_state:, cols(jj)] = jnp.where(first, tail1, tail0)
        mate2(q).start()

    def out_copies(b):
        return [
            pltpu.make_async_copy(v.at[:, lanes_of(b, jj)], h.at[:, lanes_of(b, jj)], outs.at[k])
            for k, (v, h) in enumerate([(giv, gi_hbm), (gsv, gs_hbm)])
            for jj in range(TILES)
        ]

    def differentiate(q, half):
        b = 2 * q + half
        rates = rates_of(b)

        def ahead(i, hidden):
            for s in range(SPAN):
                t = i * SPAN + s
                hs[t] = hidden
                hidden = dec[b, t] * hidden + bx[t][None] * row(uu, b, t)
                accc[t] += jnp.sum(row(gg, b, t) * hidden, axis=0)
            return hidden

        start = jnp.stack([hst[q, half, :n_state, cols(jj)] for jj in range(TILES)])
        lax.fori_loop(0, spans, ahead, start)

        def fold(slot, base):
            rows = pl.ds(pl.multiple_of(base, GROUP), GROUP)
            coeff, weigh = csp[slot, :, :GROUP], awp[slot, :, :GROUP]
            for k in range(1, SUB):
                coeff = coeff + csp[slot, :, k * GROUP : (k + 1) * GROUP]
                weigh = weigh + awp[slot, :, k * GROUP : (k + 1) * GROUP]
            cs[:, rows, :] = coeff
            ws[:, rows, :] = weigh

        def behind(i, carry):
            later, rate = carry
            base = tokens - SPAN - i * SPAN
            for slot in (1, 0):
                for s in reversed(range(GROUP)):
                    t = base + slot * GROUP + s
                    state = cx[t][None] * row(gg, b, t) + later
                    later = dec[b, t] * state
                    weighted = later * hs[t]
                    rate = rate + weighted * row(dl, b, t)
                    one, two = state * bx[t][None], weighted * rates
                    at = pl.ds(s, SUB, stride=GROUP)
                    csp[slot, :, at, :] = sum(one[:, h : h + SUB] for h in range(0, n_state, SUB))
                    awp[slot, :, at, :] = sum(two[:, h : h + SUB] for h in range(0, n_state, SUB))
                    accb[t] += jnp.sum(state * row(uu, b, t), axis=0)
                if slot:
                    fold(0, jnp.minimum(base + SPAN, tokens - GROUP))
                else:
                    fold(1, base + GROUP)
            return later, rate

        last = jnp.stack([hst[q, half, n_state:, cols(jj)] for jj in range(TILES)])
        _, rate = lax.fori_loop(0, spans, behind, (last, jnp.zeros(state_shape, F32)))
        fold(0, 0)
        for jj in range(TILES):
            lanes = lanes_of(b, jj)
            giv[:, lanes] = (dl[b, jj] * cs[jj]).astype(giv.dtype)
            gsv[:, lanes] = (xv[:, lanes].astype(F32) * cs[jj] + LN2 * ws[jj]).astype(gsv.dtype)
            rp[q, half, :, cols(jj)] = -rate[jj]
        for copy in out_copies(b):
            copy.start()

    def mate3(q):
        return remote(rp.at[q, 1 - core], rr.at[q], d3s.at[q], d3r.at[q], mate)

    def owner(q, jj, s):
        return tile_of(2 * q + core, jj) * per + s

    def rate_copy(slot, dest):
        return remote(out3.at[slot], in3.at[chip], i3s.at[slot], i3r.at[chip], dest)

    def spread(q):
        mate3(q).wait_recv()
        for jj in range(TILES):
            total = rp[q, core, :, cols(jj)] + rr[q, :, cols(jj)]
            for s in range(per):
                slot, dest = (q * TILES + jj) * per + s, owner(q, jj, s)
                out3[slot] = total[:, s * width : (s + 1) * width]

                @pl.when(dest != me)
                def _():
                    rate_copy(slot, dest).start()

                @pl.when(dest == me)
                def _():
                    in3[chip] = out3[slot]

    csp[...] = jnp.zeros_like(csp)
    awp[...] = jnp.zeros_like(awp)
    accb[...] = jnp.zeros_like(accb)
    accc[...] = jnp.zeros_like(accc)
    loads[0].wait()
    expand(bv, bx, tokens, n_state)
    loads[1].wait()
    expand(cv, cx, tokens, n_state)
    for load in loads[2:]:
        load.wait()
    own_tile, own_row = chip // share, lax.rem(chip, share) * r
    for q in range(pieces):
        mine[q] = av[:, lanes_of(2 * q + core, own_tile)] * (-LOG2E)
        for i in range(r):
            own[q, i : i + 1] = mine.at[q][pl.ds(own_row + i, SUB, stride=0), :][:1]

    def gather(q):
        summarize(q, 1 - core)

        @pl.when(q == 0)
        def _():
            pl.semaphore_wait(barrier, n - 1)

        mate1(q).start()

        @pl.when(q >= 2)
        def _():
            scan(q - 2)

        summarize(q, core)
        merge(q)

    loop(0, pieces, gather)
    split(0)

    def finish(q):
        half = lax.rem(core + (q + pieces - 1) // pieces, 2)

        @pl.when(q >= 1)
        def _():
            mate2(q).wait_recv()

        differentiate(q, half)

        @pl.when(q == 0)
        def _():
            scan(pieces - 2)
            scan(pieces - 1)
            mate2(0).wait_recv()

        @pl.when(q >= 1)
        def _():
            mate3(q).start()

        @pl.when(q == 1)
        def _():
            spread(0)

        @pl.when(q + 1 < pieces)
        def _():
            split(q + 1)

        differentiate(q, 1 - half)

        @pl.when(q == 0)
        def _():
            mate3(0).start()

        @pl.when(q >= 1)
        def _():
            spread(q)

    loop(0, pieces, finish)
    lane_sums(accb, gb_ref, tokens, n_state)
    lane_sums(accc, gc_ref, tokens, n_state)

    my_tile = me // per
    my_row = my_tile // blocks
    my_half = lax.rem(lax.rem(my_tile, blocks) + 2 * blocks - 2 * my_row, 2)

    def landed(c):
        sender = 2 * c + my_half

        @pl.when(sender != me)
        def _():
            remote(out3.at[0], in3.at[c], i3s.at[0], i3r.at[c], mate).wait_recv()

    loop(0, chips, landed)
    gr_ref[...] = lax.fori_loop(
        0, chips, lambda c, total: total + in3[c], jnp.zeros((n_state, width), F32)
    )
    for q in range(pieces):
        for copy in (mate1(q), mate2(q), mate3(q)):
            copy.wait_send()
        chip_all(out1, in1, i1s, i1r, q).wait_send()
        chip_all(out2, in2, i2s, i2r, q).wait_send()
        for jj in range(TILES):
            for s in range(per):
                slot, dest = (q * TILES + jj) * per + s, owner(q, jj, s)

                @pl.when(dest != me)
                def _():
                    rate_copy(slot, dest).wait_send()

    for k, (v, h) in enumerate([(giv, gi_hbm), (gsv, gs_hbm)]):
        pltpu.make_async_copy(v, h, outs.at[k]).wait()


def hand_out(*refs):
    count = (len(refs) - 2) // 3
    srcs, dsts, bufs = refs[:count], refs[count : 2 * count], refs[2 * count : 3 * count]
    into, away = refs[3 * count :]
    steps = []
    for k in range(count):
        rows = srcs[k].shape[0]
        parts = 4 if rows % 64 == 0 else 1
        for p in range(parts):
            steps.append((k, pl.ds(p * (rows // parts), rows // parts)))
    moves = [
        (
            pltpu.make_async_copy(srcs[k].at[part], bufs[k].at[part], into.at[i]),
            pltpu.make_async_copy(bufs[k].at[part], dsts[k].at[part], away.at[i]),
        )
        for i, (k, part) in enumerate(steps)
    ]
    for load, _ in moves:
        load.start()
    for load, store in moves:
        load.wait()
        store.start()
    for _, store in moves:
        store.wait()


def shards(n, inputs, step_sizes, cotangent, input_coeffs, output_coeffs, decay_rates):
    n_state, channels = decay_rates.shape
    tokens = inputs.shape[0]
    width = channels // n
    per = LANES // width
    chips = n // 2
    block = TILES * LANES
    blocks = channels // block
    pieces = blocks // 2
    r = n_state * TILES // chips
    assert r * chips == n_state * TILES and per * width == LANES
    wide = pltpu.VMEM((tokens, n_state, LANES), F32)
    rows = pltpu.VMEM((blocks, TILES, tokens, LANES), F32)
    part = pltpu.VMEM((TILES, tokens, LANES), F32)
    fold = pltpu.VMEM((2, TILES, GROUP * SUB, LANES), F32)
    full = pltpu.VMEM((tokens, channels), jnp.bfloat16)
    small = pltpu.VMEM((n_state, tokens), F32)
    hbm = pl.BlockSpec(memory_space=pl.ANY)
    vmem = pl.BlockSpec(memory_space=pltpu.VMEM)
    sems = pltpu.SemaphoreType.DMA((pieces,))
    outs = [
        jax.ShapeDtypeStruct((tokens, channels), jnp.bfloat16),
        jax.ShapeDtypeStruct((tokens, channels), jnp.bfloat16),
        jax.ShapeDtypeStruct((n_state, tokens), F32),
        jax.ShapeDtypeStruct((n_state, tokens), F32),
        jax.ShapeDtypeStruct((n_state, width), F32),
    ]
    results = pl.pallas_call(
        partial(whole_kernel, n),
        name="whole",
        in_specs=[hbm] * 6,
        out_specs=[hbm, hbm, vmem, vmem, vmem],
        out_shape=outs,
        scratch_shapes=[
            full, full, full, small, small, pltpu.VMEM((n_state, channels), F32), full, full,
            wide, wide, wide, wide, rows, rows, rows,
            pltpu.VMEM((blocks, tokens, TILES, n_state, LANES), F32),
            pltpu.VMEM((tokens, TILES, n_state, LANES), F32),
            fold, fold, part, part,
            pltpu.VMEM((pieces, n_state, LANES), F32),
            pltpu.VMEM((pieces, r, LANES), F32),
            pltpu.VMEM((pieces, 2, 2 * n_state + 1, block), F32),
            pltpu.VMEM((pieces, 2 * n_state + 1, block), F32),
            pltpu.VMEM((pieces, chips, 2 * r + 1, LANES), F32),
            pltpu.VMEM((pieces, chips, 2 * r + 1, LANES), F32),
            pltpu.VMEM((pieces, chips, 2 * r, LANES), F32),
            pltpu.VMEM((pieces, chips, 2 * r, LANES), F32),
            pltpu.VMEM((2 * n_state, block), F32),
            pltpu.VMEM((pieces, 2 * n_state, block), F32),
            pltpu.VMEM((pieces, 2, 2 * n_state, block), F32),
            pltpu.VMEM((pieces, 2, n_state, block), F32),
            pltpu.VMEM((pieces, n_state, block), F32),
            pltpu.VMEM((pieces * TILES * per, n_state, width), F32),
            pltpu.VMEM((chips, n_state, width), F32),
            pltpu.SemaphoreType.DMA((6,)), pltpu.SemaphoreType.DMA((2,)),
            sems, sems, sems, sems, sems, sems, sems, sems, sems, sems,
            pltpu.SemaphoreType.DMA((pieces * TILES * per,)),
            pltpu.SemaphoreType.DMA((chips,)),
        ],
        compiler_params=pltpu.CompilerParams(
            collective_id=0, has_side_effects=True, vmem_limit_bytes=63 * 1024 * 1024
        ),
    )(inputs, step_sizes, cotangent, input_coeffs, output_coeffs, decay_rates)
    moves = 11
    return pl.pallas_call(
        hand_out,
        name="hand_out",
        in_specs=[hbm] * 5,
        out_specs=[hbm] * 5,
        out_shape=outs,
        scratch_shapes=[
            *[pltpu.VMEM(o.shape, o.dtype) for o in outs],
            pltpu.SemaphoreType.DMA((moves,)), pltpu.SemaphoreType.DMA((moves,)),
        ],
    )(*results)


def solution(mesh):
    placed = (P("seq", None), P("seq", None), P("seq", None), P(None, "seq"), P(None, "seq"), P())
    return jax.shard_map(
        partial(shards, mesh.shape["seq"]),
        mesh=mesh,
        in_specs=placed,
        out_specs=(P("seq", None), P("seq", None), P(None, "seq"), P(None, "seq"), P(None, "seq")),
        check_vma=False,
    )
```

```python
from functools import partial
import math

import jax
import jax.numpy as jnp
from jax import lax
from jax.experimental import pallas as pl
from jax.experimental.pallas import tpu as pltpu
from jax.sharding import PartitionSpec as P

LANES = 128
SUB = 8
TILES = 4
GROUP = 8
SPAN = 16
STRIDE = 32
LOG2E = math.log2(math.e)
LN2 = math.log(2.0)
F32 = jnp.float32
MESH = pl.DeviceIdType.MESH


def loop(start, stop, body):
    def step(k, _):
        body(k)
        return 0

    lax.fori_loop(start, stop, step, 0)


def expand(coef_ref, wide, tokens, n_state):
    for t in range(tokens):
        wide[t] = jnp.broadcast_to(coef_ref[:, t : t + 1], (n_state, LANES))


def lane_sums(acc, out_ref, tokens, n_state):
    lane = lax.broadcasted_iota(jnp.int32, (n_state, tokens), 1)
    total = jnp.zeros((n_state, tokens), F32)
    for t in range(tokens):
        total = jnp.where(lane == t, jnp.sum(acc[t], axis=1, keepdims=True), total)
    out_ref[...] = total


def cols(jj):
    return slice(jj * LANES, (jj + 1) * LANES)


def whole_kernel(
    n,
    x_hbm, d_hbm, g_hbm, b_hbm, c_hbm, a_hbm,
    gi_hbm, gs_hbm, gb_ref, gc_ref, gr_ref,
    xv, dv, gv, bv, cv, av, giv, gsv,
    bx, cx, accb, accc, dl, uu, gg, dec, hs, csp, awp, cs, ws, mine, own,
    sm, rv, out1, in1, out2, in2, st2, tmp, hst, rp, rr, out3, in3,
    ins, outs, d1s, d1r, i1s, i1r, i2s, i2r, d2s, d2r, d3s, d3r, i3s, i3r,
):
    me = lax.axis_index("seq")
    core, chip = lax.rem(me, 2), me // 2
    mate = 2 * chip + 1 - core
    tokens, channels = xv.shape
    n_state = av.shape[0]
    chips = n // 2
    blocks = channels // (LANES * TILES)
    pieces = blocks // 2
    share = chips // TILES
    r = n_state // share
    width = channels // n
    per = LANES // width
    first = core == 0
    barrier = pltpu.get_barrier_semaphore()

    loads = [
        pltpu.make_async_copy(src, dst, ins.at[k])
        for k, (src, dst) in enumerate(
            [(b_hbm, bv), (c_hbm, cv), (d_hbm, dv), (x_hbm, xv), (g_hbm, gv), (a_hbm, av)]
        )
    ]
    for load in loads:
        load.start()

    pace = 2 if per == 1 else 1

    def tell(dest):
        pl.semaphore_signal(barrier, inc=1, device_id=(dest,), device_id_type=MESH)

    loop(1, n // pace, lambda k: tell(lax.rem(me + pace * k, n)))
    if pace == 2:
        tell(mate)

    def tile_of(b, jj):
        return blocks * jj + lax.rem(b + 2 * jj, blocks)

    def lanes_of(b, jj):
        return pl.ds(pl.multiple_of(tile_of(b, jj) * LANES, LANES), LANES)

    def remote(src, dst, send_sem, recv_sem, dest):
        return pltpu.make_async_remote_copy(
            src_ref=src, dst_ref=dst, send_sem=send_sem, recv_sem=recv_sem,
            device_id=(dest,), device_id_type=MESH,
        )

    def row(ref, b, t):
        return ref.at[b][:, pl.ds(t, n_state, stride=0), :]

    def rates_of(b):
        return jnp.stack([av[:, lanes_of(b, jj)] * (-LOG2E) for jj in range(TILES)])

    state_shape = (TILES, n_state, LANES)
    spans = tokens // SPAN

    def summarize(q, half):
        b = 2 * q + half
        for jj in range(TILES):
            lanes = lanes_of(b, jj)
            delta = dv[:, lanes].astype(F32)
            dl[b, jj] = delta
            uu[b, jj] = delta * xv[:, lanes].astype(F32)
            gg[b, jj] = gv[:, lanes].astype(F32)
            sm[q, half, 2 * n_state :, cols(jj)] = jnp.sum(delta, axis=0, keepdims=True)
        rates = rates_of(b)

        def ahead(i, end):
            for s in range(STRIDE):
                t = i * STRIDE + s
                decay = jnp.exp2(row(dl, b, t) * rates)
                dec[b, t] = decay
                end = decay * end + bx[t][None] * row(uu, b, t)
            return end

        def behind(i, back):
            for s in reversed(range(SPAN)):
                t = tokens - SPAN - i * SPAN + s
                accb[t] = clear
                accc[t] = clear
                back = dec[b, t] * (cx[t][None] * row(gg, b, t) + back)
            return back

        zero, clear = jnp.zeros(state_shape, F32), jnp.zeros((n_state, LANES), F32)
        end = lax.fori_loop(0, tokens // STRIDE, ahead, zero)
        back = lax.fori_loop(0, spans, behind, zero)
        for jj in range(TILES):
            sm[q, half, :n_state, cols(jj)] = end[jj]
            sm[q, half, n_state : 2 * n_state, cols(jj)] = back[jj]

    def mate1(q):
        return remote(sm.at[q, 1 - core], rv.at[q], d1s.at[q], d1r.at[q], mate)

    def pair_of(q, jj):
        rates = av[:, lanes_of(2 * q + core, jj)] * (-LOG2E)
        kept = sm.at[q, core]
        end_m, back_m = kept[:n_state, cols(jj)], kept[n_state : 2 * n_state, cols(jj)]
        sum_m = kept[2 * n_state :, cols(jj)]
        end_t, back_t = rv[q, :n_state, cols(jj)], rv[q, n_state : 2 * n_state, cols(jj)]
        sum_t = rv[q, 2 * n_state :, cols(jj)]
        pick = lambda a, b: (jnp.where(first, a, b), jnp.where(first, b, a))
        return rates, pick(end_m, end_t), pick(back_m, back_t), pick(sum_m, sum_t)

    def chip_copy(src, dst, send_sem, recv_sem, q, there):
        return remote(
            src.at[q, there], dst.at[q, chip], send_sem.at[q], recv_sem.at[q], 2 * there + core
        )

    def chip_sends(*refs):
        def send(k):
            chip_copy(*refs, lax.rem(chip + k, chips)).start()

        loop(1, chips, send)

    def chip_all(src, dst, send_sem, recv_sem, q):
        part = pl.ds(0, chips - 1)
        return remote(src.at[q, part], dst.at[q, part], send_sem.at[q], recv_sem.at[q], mate)

    def merge(q):
        mate1(q).wait_recv()
        for jj in range(TILES):
            rates, (end0, end1), (back0, back1), (sum0, sum1) = pair_of(q, jj)
            end = jnp.exp2(rates * sum1) * end0 + end1
            back = back0 + jnp.exp2(rates * sum0) * back1
            for i in range(share):
                slot, rows = jj * share + i, slice(i * r, (i + 1) * r)
                out1[q, slot, :r] = end[rows]
                out1[q, slot, r : 2 * r] = back[rows]
                out1[q, slot, 2 * r :] = sum0 + sum1
        in1[q, chip] = out1[q, chip]
        chip_sends(out1, in1, i1s, i1r, q)

    def scan(q):
        chip_all(out1, in1, i1s, i1r, q).wait_recv()
        rates = own[q]

        def step(c, carry):
            ahead, behind = carry
            e = chips - 1 - c
            out2[q, c, :r] = ahead
            out2[q, e, r:] = behind
            ahead = jnp.exp2(rates * in1[q, c, 2 * r :]) * ahead + in1[q, c, :r]
            behind = jnp.exp2(rates * in1[q, e, 2 * r :]) * behind + in1[q, e, r : 2 * r]
            return ahead, behind

        blank = jnp.zeros((r, LANES), F32)
        lax.fori_loop(0, chips, step, (blank, blank), unroll=8)
        in2[q, chip] = out2[q, chip]
        chip_sends(out2, in2, i2s, i2r, q)

    def mate2(q):
        return remote(tmp.at[q], hst.at[q, core], d2s.at[q], d2r.at[q], mate)

    def split(q):
        chip_all(out2, in2, i2s, i2r, q).wait_recv()
        for jj in range(TILES):
            for i in range(share):
                slot, at = jj * share + i, i * r
                st2[at : at + r, cols(jj)] = in2[q, slot, :r]
                st2[n_state + at : n_state + at + r, cols(jj)] = in2[q, slot, r:]
        for jj in range(TILES):
            rates, (end0, _), (_, back1), (sum0, sum1) = pair_of(q, jj)
            head0, tail1 = st2[:n_state, cols(jj)], st2[n_state:, cols(jj)]
            head1 = jnp.exp2(rates * sum0) * head0 + end0
            tail0 = jnp.exp2(rates * sum1) * tail1 + back1
            hst[q, core, :n_state, cols(jj)] = jnp.where(first, head0, head1)
            hst[q, core, n_state:, cols(jj)] = jnp.where(first, tail0, tail1)
            tmp[q, :n_state, cols(jj)] = jnp.where(first, head1, head0)
            tmp[q, n_state:, cols(jj)] = jnp.where(first, tail1, tail0)
        mate2(q).start()

    def out_copies(b):
        return [
            pltpu.make_async_copy(v.at[:, lanes_of(b, jj)], h.at[:, lanes_of(b, jj)], outs.at[k])
            for k, (v, h) in enumerate([(giv, gi_hbm), (gsv, gs_hbm)])
            for jj in range(TILES)
        ]

    def differentiate(q, half, between=None):
        b = 2 * q + half
        rates = rates_of(b)

        def ahead(i, hidden):
            for s in range(STRIDE):
                t = i * STRIDE + s
                hs[t] = hidden
                hidden = dec[b, t] * hidden + bx[t][None] * row(uu, b, t)
                accc[t] += jnp.sum(row(gg, b, t) * hidden, axis=0)
            return hidden

        start = jnp.stack([hst[q, half, :n_state, cols(jj)] for jj in range(TILES)])
        lax.fori_loop(0, tokens // STRIDE, ahead, start)

        def fold(slot, base):
            rows = pl.ds(pl.multiple_of(base, GROUP), GROUP)
            parts = [pl.ds(k * (GROUP + 1), GROUP) for k in range(SUB)]
            cs[:, rows, :] = sum(csp[slot, :, part] for part in parts)
            ws[:, rows, :] = sum(awp[slot, :, part] for part in parts)

        def behind(chain, sums, i, carry):
            later, rate = carry
            base = tokens - SPAN - i * SPAN
            for slot in (1, 0):
                for s in reversed(range(GROUP)):
                    t = base + slot * GROUP + s
                    if chain:
                        state = cx[t][None] * row(gg, b, t) + later
                        later = dec[b, t] * state
                        weighted = later * hs[t]
                        rate = rate + weighted * row(dl, b, t)
                    else:
                        state, weighted = dec[b, t], hs[t]
                    if chain and not sums:
                        dec[b, t] = state
                        hs[t] = weighted
                    if sums:
                        one, two = state * bx[t][None], weighted * rates
                        at = pl.ds(s, SUB, stride=GROUP + 1)
                        csp[slot, :, at, :] = sum(one[:, h : h + SUB] for h in range(0, n_state, SUB))
                        awp[slot, :, at, :] = sum(two[:, h : h + SUB] for h in range(0, n_state, SUB))
                        accb[t] += jnp.sum(state * row(uu, b, t), axis=0)
                if sums and slot:
                    fold(0, jnp.minimum(base + SPAN, tokens - GROUP))
                elif sums:
                    fold(1, base + GROUP)
            return later, rate

        last = jnp.stack([hst[q, half, n_state:, cols(jj)] for jj in range(TILES)])
        carry = (last, jnp.zeros(state_shape, F32))
        _, rate = lax.fori_loop(0, spans, partial(behind, True, between is None), carry)
        for jj in range(TILES):
            rp[q, half, :, cols(jj)] = -rate[jj]
        if between is not None:
            between()
            lax.fori_loop(0, spans, partial(behind, False, True), (0, 0))
        fold(0, 0)
        for jj in range(TILES):
            lanes = lanes_of(b, jj)
            giv[:, lanes] = (dl[b, jj] * cs[jj]).astype(giv.dtype)
            gsv[:, lanes] = (xv[:, lanes].astype(F32) * cs[jj] + LN2 * ws[jj]).astype(gsv.dtype)
        for copy in out_copies(b):
            copy.start()

    def mate3(q):
        return remote(rp.at[q, 1 - core], rr.at[q], d3s.at[q], d3r.at[q], mate)

    def owner(q, jj, s):
        return tile_of(2 * q + core, jj) * per + s

    def rate_copy(slot, dest):
        return remote(out3.at[slot], in3.at[chip], i3s.at[slot], i3r.at[chip], dest)

    def spread(q):
        mate3(q).wait_recv()
        for jj in range(TILES):
            total = rp[q, core, :, cols(jj)] + rr[q, :, cols(jj)]
            for s in range(per):
                slot, dest = (q * TILES + jj) * per + s, owner(q, jj, s)
                out3[slot] = total[:, s * width : (s + 1) * width]

                @pl.when(dest != me)
                def _():
                    rate_copy(slot, dest).start()

                @pl.when(dest == me)
                def _():
                    in3[chip] = out3[slot]

    csp[0] = jnp.zeros(csp.shape[1:], F32)
    awp[0] = jnp.zeros(awp.shape[1:], F32)
    loads[0].wait()
    expand(bv, bx, tokens, n_state)
    loads[1].wait()
    expand(cv, cx, tokens, n_state)
    for load in loads[2:]:
        load.wait()
    own_tile, own_row = chip // share, lax.rem(chip, share) * r
    for q in range(pieces):
        mine[q] = av[:, lanes_of(2 * q + core, own_tile)] * (-LOG2E)
        for i in range(r):
            own[q, i : i + 1] = mine.at[q][pl.ds(own_row + i, SUB, stride=0), :][:1]

    def gather(u):
        q, odd = u // 2, lax.rem(u, 2)
        summarize(q, lax.rem(1 - core + odd, 2))

        @pl.when(u == 0)
        def _():
            pl.semaphore_wait(barrier, n // pace - 1 + (pace == 2))

        @pl.when(odd == 0)
        def _():
            mate1(q).start()

            @pl.when(q >= 2)
            def _():
                scan(q - 2)

        @pl.when(odd == 1)
        def _():
            merge(q)

    loop(0, 2 * pieces, gather)
    split(0)

    def finish(u):
        q, odd = u // 2, lax.rem(u, 2)
        differentiate(q, lax.rem(core + odd + (q + pieces - 1) // pieces, 2))

        @pl.when(u == 0)
        def _():
            scan(pieces - 2)
            scan(pieces - 1)
            mate2(0).wait_recv()

        @pl.when(odd + 2 * q == 1)
        def _():
            mate3(0).start()

        @pl.when((1 - odd) * q >= 1)
        def _():
            mate3(q).start()

        @pl.when(u == 2)
        def _():
            spread(0)

        @pl.when(odd * q >= 1)
        def _():
            spread(q)

        @pl.when(q + 1 < pieces)
        def _():
            @pl.when(odd == 0)
            def _():
                split(q + 1)

            @pl.when(odd == 1)
            def _():
                mate2(q + 1).wait_recv()

    loop(0, 2 * pieces - 1, finish)
    differentiate(pieces - 1, core, lambda: spread(pieces - 1))
    lane_sums(accb, gb_ref, tokens, n_state)
    lane_sums(accc, gc_ref, tokens, n_state)

    my_tile = me // per
    my_row = my_tile // blocks
    my_half = lax.rem(lax.rem(my_tile, blocks) + 2 * blocks - 2 * my_row, 2)

    def landed(c):
        sender = 2 * c + my_half

        @pl.when(sender != me)
        def _():
            remote(out3.at[0], in3.at[c], i3s.at[0], i3r.at[c], mate).wait_recv()

    loop(0, chips, landed)
    gr_ref[...] = lax.fori_loop(
        0, chips, lambda c, total: total + in3[c], jnp.zeros((n_state, width), F32)
    )
    for q in range(pieces):
        for copy in (mate1(q), mate2(q), mate3(q)):
            copy.wait_send()
        chip_all(out1, in1, i1s, i1r, q).wait_send()
        chip_all(out2, in2, i2s, i2r, q).wait_send()
        for jj in range(TILES):
            for s in range(per):
                slot, dest = (q * TILES + jj) * per + s, owner(q, jj, s)

                @pl.when(dest != me)
                def _():
                    rate_copy(slot, dest).wait_send()

    for k, (v, h) in enumerate([(giv, gi_hbm), (gsv, gs_hbm)]):
        pltpu.make_async_copy(v, h, outs.at[k]).wait()


def hand_out(*refs):
    count = (len(refs) - 2) // 3
    srcs, dsts, bufs = refs[:count], refs[count : 2 * count], refs[2 * count : 3 * count]
    into, away = refs[3 * count :]
    steps = []
    for k in range(count):
        rows = srcs[k].shape[0]
        parts = 4 if rows % 64 == 0 else 1
        for p in range(parts):
            steps.append((k, pl.ds(p * (rows // parts), rows // parts)))
    moves = [
        (
            pltpu.make_async_copy(srcs[k].at[part], bufs[k].at[part], into.at[i]),
            pltpu.make_async_copy(bufs[k].at[part], dsts[k].at[part], away.at[i]),
        )
        for i, (k, part) in enumerate(steps)
    ]
    for load, _ in moves:
        load.start()
    for load, store in moves:
        load.wait()
        store.start()
    for _, store in moves:
        store.wait()


def shards(n, inputs, step_sizes, cotangent, input_coeffs, output_coeffs, decay_rates):
    n_state, channels = decay_rates.shape
    tokens = inputs.shape[0]
    width = channels // n
    per = LANES // width
    chips = n // 2
    block = TILES * LANES
    blocks = channels // block
    pieces = blocks // 2
    r = n_state * TILES // chips
    assert r * chips == n_state * TILES and per * width == LANES
    wide = pltpu.VMEM((tokens, n_state, LANES), F32)
    rows = pltpu.VMEM((blocks, TILES, tokens, LANES), F32)
    part = pltpu.VMEM((TILES, tokens, LANES), F32)
    fold = pltpu.VMEM((2, TILES, (GROUP + 1) * SUB, LANES), F32)
    full = pltpu.VMEM((tokens, channels), jnp.bfloat16)
    small = pltpu.VMEM((n_state, tokens), F32)
    hbm = pl.BlockSpec(memory_space=pl.ANY)
    vmem = pl.BlockSpec(memory_space=pltpu.VMEM)
    sems = pltpu.SemaphoreType.DMA((pieces,))
    outs = [
        jax.ShapeDtypeStruct((tokens, channels), jnp.bfloat16),
        jax.ShapeDtypeStruct((tokens, channels), jnp.bfloat16),
        jax.ShapeDtypeStruct((n_state, tokens), F32),
        jax.ShapeDtypeStruct((n_state, tokens), F32),
        jax.ShapeDtypeStruct((n_state, width), F32),
    ]
    results = pl.pallas_call(
        partial(whole_kernel, n),
        name="whole",
        in_specs=[hbm] * 6,
        out_specs=[hbm, hbm, vmem, vmem, vmem],
        out_shape=outs,
        scratch_shapes=[
            full, full, full, small, small, pltpu.VMEM((n_state, channels), F32), full, full,
            wide, wide, wide, wide, rows, rows, rows,
            pltpu.VMEM((blocks, tokens, TILES, n_state, LANES), F32),
            pltpu.VMEM((tokens, TILES, n_state, LANES), F32),
            fold, fold, part, part,
            pltpu.VMEM((pieces, n_state, LANES), F32),
            pltpu.VMEM((pieces, r, LANES), F32),
            pltpu.VMEM((pieces, 2, 2 * n_state + 1, block), F32),
            pltpu.VMEM((pieces, 2 * n_state + 1, block), F32),
            pltpu.VMEM((pieces, chips, 2 * r + 1, LANES), F32),
            pltpu.VMEM((pieces, chips, 2 * r + 1, LANES), F32),
            pltpu.VMEM((pieces, chips, 2 * r, LANES), F32),
            pltpu.VMEM((pieces, chips, 2 * r, LANES), F32),
            pltpu.VMEM((2 * n_state, block), F32),
            pltpu.VMEM((pieces, 2 * n_state, block), F32),
            pltpu.VMEM((pieces, 2, 2 * n_state, block), F32),
            pltpu.VMEM((pieces, 2, n_state, block), F32),
            pltpu.VMEM((pieces, n_state, block), F32),
            pltpu.VMEM((pieces * TILES * per, n_state, width), F32),
            pltpu.VMEM((chips, n_state, width), F32),
            pltpu.SemaphoreType.DMA((6,)), pltpu.SemaphoreType.DMA((2,)),
            sems, sems, sems, sems, sems, sems, sems, sems, sems, sems,
            pltpu.SemaphoreType.DMA((pieces * TILES * per,)),
            pltpu.SemaphoreType.DMA((chips,)),
        ],
        compiler_params=pltpu.CompilerParams(
            collective_id=0, has_side_effects=True, vmem_limit_bytes=63 * 1024 * 1024
        ),
    )(inputs, step_sizes, cotangent, input_coeffs, output_coeffs, decay_rates)
    moves = 11
    return pl.pallas_call(
        hand_out,
        name="hand_out",
        in_specs=[hbm] * 5,
        out_specs=[hbm] * 5,
        out_shape=outs,
        scratch_shapes=[
            *[pltpu.VMEM(o.shape, o.dtype) for o in outs],
            pltpu.SemaphoreType.DMA((moves,)), pltpu.SemaphoreType.DMA((moves,)),
        ],
    )(*results)


def solution(mesh):
    placed = (P("seq", None), P("seq", None), P("seq", None), P(None, "seq"), P(None, "seq"), P())
    return jax.shard_map(
        partial(shards, mesh.shape["seq"]),
        mesh=mesh,
        in_specs=placed,
        out_specs=(P("seq", None), P("seq", None), P(None, "seq"), P(None, "seq"), P(None, "seq")),
        check_vma=False,
    )
```

```python
from functools import partial
import math

import jax
import jax.numpy as jnp
from jax import lax
from jax.experimental import pallas as pl
from jax.experimental.pallas import tpu as pltpu
from jax.sharding import PartitionSpec as P

LANES = 128
SUB = 8
TILES = 4
GROUP = 8
SPAN = 16
STRIDE = 32
LOG2E = math.log2(math.e)
LN2 = math.log(2.0)
F32 = jnp.float32
MESH = pl.DeviceIdType.MESH


def loop(start, stop, body):
    def step(k, _):
        body(k)
        return 0

    lax.fori_loop(start, stop, step, 0)


def expand(coef_ref, wide, tokens, n_state):
    for t in range(tokens):
        wide[t] = jnp.broadcast_to(coef_ref[:, t : t + 1], (n_state, LANES))


def lane_sums(acc, out_ref, tokens, n_state):
    lane = lax.broadcasted_iota(jnp.int32, (n_state, tokens), 1)
    total = jnp.zeros((n_state, tokens), F32)
    for t in range(tokens):
        total = jnp.where(lane == t, jnp.sum(acc[t], axis=1, keepdims=True), total)
    out_ref[...] = total


def cols(jj):
    return slice(jj * LANES, (jj + 1) * LANES)


def whole_kernel(
    n,
    x_hbm, d_hbm, g_hbm, b_hbm, c_hbm, a_hbm,
    giv, gsv, gb_ref, gc_ref, gr_ref,
    xv, dv, gv, bv, cv, av,
    bx, cx, accb, accc, dl, uu, gg, dec, hs, csp, awp, cs, ws, mine, own,
    sm, rv, out1, in1, out2, in2, st2, tmp, hst, rp, rr, out3, in3,
    ins, d1s, d1r, i1s, i1r, i2s, i2r, d2s, d2r, d3s, d3r, i3s, i3r,
):
    me = lax.axis_index("seq")
    core, chip = lax.rem(me, 2), me // 2
    mate = 2 * chip + 1 - core
    tokens, channels = xv.shape
    n_state = av.shape[0]
    chips = n // 2
    blocks = channels // (LANES * TILES)
    pieces = blocks // 2
    share = chips // TILES
    r = n_state // share
    width = channels // n
    per = LANES // width
    first = core == 0
    barrier = pltpu.get_barrier_semaphore()

    coefs = [
        pltpu.make_async_copy(src, dst, ins.at[k])
        for k, (src, dst) in enumerate([(b_hbm, bv), (c_hbm, cv), (a_hbm, av)])
    ]
    bulk = [(d_hbm, dv), (x_hbm, xv), (g_hbm, gv)]
    starts = [(blocks + 2) * jj for jj in range(TILES)]

    def load(k, sem, tile, count):
        at = pl.ds(tile * LANES, count * LANES)
        src, dst = bulk[k]
        return pltpu.make_async_copy(src.at[:, at], dst.at[:, at], ins.at[sem])

    for copy in coefs:
        copy.start()
    for k in range(3):
        for tile in starts:
            load(k, 3 + k, tile, 2).start()
    for k in range(3):
        for tile in starts[:-1]:
            load(k, 6 + k, tile + 2, blocks).start()

    pace = 2 if per == 1 else 1

    def tell(dest):
        pl.semaphore_signal(barrier, inc=1, device_id=(dest,), device_id_type=MESH)

    loop(1, n // pace, lambda k: tell(lax.rem(me + pace * k, n)))
    if pace == 2:
        tell(mate)

    def tile_of(b, jj):
        return blocks * jj + lax.rem(b + 2 * jj, blocks)

    def lanes_of(b, jj):
        return pl.ds(pl.multiple_of(tile_of(b, jj) * LANES, LANES), LANES)

    def remote(src, dst, send_sem, recv_sem, dest):
        return pltpu.make_async_remote_copy(
            src_ref=src, dst_ref=dst, send_sem=send_sem, recv_sem=recv_sem,
            device_id=(dest,), device_id_type=MESH,
        )

    def row(ref, b, t):
        return ref.at[b][:, pl.ds(t, n_state, stride=0), :]

    def rates_of(b):
        return jnp.stack([av[:, lanes_of(b, jj)] * (-LOG2E) for jj in range(TILES)])

    state_shape = (TILES, n_state, LANES)
    spans = tokens // SPAN

    def summarize(q, half):
        b = 2 * q + half
        for jj in range(TILES):
            lanes = lanes_of(b, jj)
            delta = dv[:, lanes].astype(F32)
            dl[b, jj, :tokens] = delta
            uu[b, jj, :tokens] = delta * xv[:, lanes].astype(F32)
            gg[b, jj, :tokens] = gv[:, lanes].astype(F32)
            sm[q, half, 2 * n_state :, cols(jj)] = jnp.sum(delta, axis=0, keepdims=True)
        rates = rates_of(b)

        def ahead(i, end):
            for s in range(STRIDE):
                t = i * STRIDE + s
                decay = jnp.exp2(row(dl, b, t) * rates)
                dec[b, t] = decay
                end = decay * end + bx[t][None] * row(uu, b, t)
            return end

        def behind(i, back):
            for s in reversed(range(SPAN)):
                t = tokens - SPAN - i * SPAN + s
                accb[t] = clear
                accc[t] = clear
                back = dec[b, t] * (cx[t][None] * row(gg, b, t) + back)
            return back

        zero, clear = jnp.zeros(state_shape, F32), jnp.zeros((n_state, LANES), F32)
        end = lax.fori_loop(0, tokens // STRIDE, ahead, zero)
        back = lax.fori_loop(0, spans, behind, zero)
        for jj in range(TILES):
            sm[q, half, :n_state, cols(jj)] = end[jj]
            sm[q, half, n_state : 2 * n_state, cols(jj)] = back[jj]

    def mate1(q):
        return remote(sm.at[q, 1 - core], rv.at[q], d1s.at[q], d1r.at[q], mate)

    def pair_of(q, jj):
        rates = av[:, lanes_of(2 * q + core, jj)] * (-LOG2E)
        kept = sm.at[q, core]
        end_m, back_m = kept[:n_state, cols(jj)], kept[n_state : 2 * n_state, cols(jj)]
        sum_m = kept[2 * n_state :, cols(jj)]
        end_t, back_t = rv[q, :n_state, cols(jj)], rv[q, n_state : 2 * n_state, cols(jj)]
        sum_t = rv[q, 2 * n_state :, cols(jj)]
        pick = lambda a, b: (jnp.where(first, a, b), jnp.where(first, b, a))
        return rates, pick(end_m, end_t), pick(back_m, back_t), pick(sum_m, sum_t)

    def chip_copy(src, dst, send_sem, recv_sem, q, there):
        return remote(
            src.at[q, there], dst.at[q, chip], send_sem.at[q], recv_sem.at[q], 2 * there + core
        )

    def chip_sends(*refs):
        def send(k):
            chip_copy(*refs, lax.rem(chip + k, chips)).start()

        loop(1, chips, send)

    def chip_all(src, dst, send_sem, recv_sem, q):
        part = pl.ds(0, chips - 1)
        return remote(src.at[q, part], dst.at[q, part], send_sem.at[q], recv_sem.at[q], mate)

    def merge(q):
        mate1(q).wait_recv()
        for jj in range(TILES):
            rates, (end0, end1), (back0, back1), (sum0, sum1) = pair_of(q, jj)
            end = jnp.exp2(rates * sum1) * end0 + end1
            back = back0 + jnp.exp2(rates * sum0) * back1
            for i in range(share):
                slot, rows = jj * share + i, slice(i * r, (i + 1) * r)
                out1[q, slot, :r] = end[rows]
                out1[q, slot, r : 2 * r] = back[rows]
                out1[q, slot, 2 * r :] = sum0 + sum1
        in1[q, chip] = out1[q, chip]
        chip_sends(out1, in1, i1s, i1r, q)

    def scan(q):
        chip_all(out1, in1, i1s, i1r, q).wait_recv()
        rates = own[q]

        def step(c, carry):
            ahead, behind = carry
            e = chips - 1 - c
            out2[q, c, :r] = ahead
            out2[q, e, r:] = behind
            ahead = jnp.exp2(rates * in1[q, c, 2 * r :]) * ahead + in1[q, c, :r]
            behind = jnp.exp2(rates * in1[q, e, 2 * r :]) * behind + in1[q, e, r : 2 * r]
            return ahead, behind

        blank = jnp.zeros((r, LANES), F32)
        lax.fori_loop(0, chips, step, (blank, blank), unroll=8)
        in2[q, chip] = out2[q, chip]
        chip_sends(out2, in2, i2s, i2r, q)

    def mate2(q):
        return remote(tmp.at[q], hst.at[q, core], d2s.at[q], d2r.at[q], mate)

    def split(q):
        chip_all(out2, in2, i2s, i2r, q).wait_recv()
        for jj in range(TILES):
            for i in range(share):
                slot, at = jj * share + i, i * r
                st2[at : at + r, cols(jj)] = in2[q, slot, :r]
                st2[n_state + at : n_state + at + r, cols(jj)] = in2[q, slot, r:]
        for jj in range(TILES):
            rates, (end0, _), (_, back1), (sum0, sum1) = pair_of(q, jj)
            head0, tail1 = st2[:n_state, cols(jj)], st2[n_state:, cols(jj)]
            head1 = jnp.exp2(rates * sum0) * head0 + end0
            tail0 = jnp.exp2(rates * sum1) * tail1 + back1
            hst[q, core, :n_state, cols(jj)] = jnp.where(first, head0, head1)
            hst[q, core, n_state:, cols(jj)] = jnp.where(first, tail0, tail1)
            tmp[q, :n_state, cols(jj)] = jnp.where(first, head1, head0)
            tmp[q, n_state:, cols(jj)] = jnp.where(first, tail1, tail0)
        mate2(q).start()

    def forward(q, half, slot):
        b = 2 * q + half
        held = hs.at[slot]

        def ahead(i, hidden):
            for s in range(STRIDE):
                t = i * STRIDE + s
                held[t] = hidden
                hidden = dec[b, t] * hidden + bx[t][None] * row(uu, b, t)
                accc[t] += jnp.sum(row(gg, b, t) * hidden, axis=0)
            return hidden

        start = jnp.stack([hst[q, half, :n_state, cols(jj)] for jj in range(TILES)])
        lax.fori_loop(0, tokens // STRIDE, ahead, start)

    def fold(slot, base):
        rows = pl.ds(pl.multiple_of(base, GROUP), GROUP)
        parts = [pl.ds(k * (GROUP + 1), GROUP) for k in range(SUB)]
        cs[:, rows, :] = sum(csp[slot, :, part] for part in parts)
        ws[:, rows, :] = sum(awp[slot, :, part] for part in parts)

    def backward(q, half, place, chain, sums):
        b = 2 * q + half
        held = hs.at[place]
        rates = rates_of(b)

        def halves(x):
            return sum(x[:, h : h + SUB] for h in range(0, n_state, SUB))

        def behind(i, carry):
            later, rate = carry
            base = tokens - SPAN - i * SPAN
            for slot in (1, 0):
                for s in reversed(range(GROUP)):
                    t = base + slot * GROUP + s
                    if chain:
                        state = cx[t][None] * row(gg, b, t) + later
                        later = dec[b, t] * state
                        weighted = later * held[t]
                        rate = rate + weighted * row(dl, b, t)
                    else:
                        state, weighted = dec[b, t], held[t]
                    if sums:
                        at = pl.ds(s, SUB, stride=GROUP + 1)
                        csp[slot, :, at, :] = halves(state * bx[t][None])
                        awp[slot, :, at, :] = halves(weighted * rates)
                        accb[t] += jnp.sum(state * row(uu, b, t), axis=0)
                    else:
                        dec[b, t] = state
                        held[t] = weighted
                if sums and slot:
                    fold(0, jnp.minimum(base + SPAN, tokens - GROUP))
                elif sums:
                    fold(1, base + GROUP)
            return later, rate

        last = jnp.stack([hst[q, half, n_state:, cols(jj)] for jj in range(TILES)])
        carry = (last, jnp.zeros(state_shape, F32)) if chain else (0, 0)
        _, rate = lax.fori_loop(0, spans, behind, carry)
        if chain:
            for jj in range(TILES):
                rp[q, half, :, cols(jj)] = -rate[jj]
        if sums:
            fold(0, 0)
            for jj in range(TILES):
                lanes = lanes_of(b, jj)
                giv[:, lanes] = (dl[b, jj, :tokens] * cs[jj]).astype(giv.dtype)
                x = xv[:, lanes].astype(F32)
                gsv[:, lanes] = (x * cs[jj] + LN2 * ws[jj]).astype(gsv.dtype)

    def mate3(q):
        return remote(rp.at[q, 1 - core], rr.at[q], d3s.at[q], d3r.at[q], mate)

    def owner(q, jj, s):
        return tile_of(2 * q + core, jj) * per + s

    def rate_copy(slot, dest):
        return remote(out3.at[slot], in3.at[chip], i3s.at[slot], i3r.at[chip], dest)

    def spread(q):
        mate3(q).wait_recv()
        for jj in range(TILES):
            total = rp[q, core, :, cols(jj)] + rr[q, :, cols(jj)]
            for s in range(per):
                slot, dest = (q * TILES + jj) * per + s, owner(q, jj, s)
                out3[slot] = total[:, s * width : (s + 1) * width]

                @pl.when(dest != me)
                def _():
                    rate_copy(slot, dest).start()

                @pl.when(dest == me)
                def _():
                    in3[chip] = out3[slot]

    csp[0] = jnp.zeros(csp.shape[1:], F32)
    awp[0] = jnp.zeros(awp.shape[1:], F32)
    coefs[0].wait()
    expand(bv, bx, tokens, n_state)
    coefs[1].wait()
    expand(cv, cx, tokens, n_state)
    coefs[2].wait()
    for k in range(3):
        load(k, 3 + k, 0, 2 * TILES).wait()
    own_tile, own_row = chip // share, lax.rem(chip, share) * r
    for q in range(pieces):
        mine[q] = av[:, lanes_of(2 * q + core, own_tile)] * (-LOG2E)
        for i in range(r):
            own[q, i : i + 1] = mine.at[q][pl.ds(own_row + i, SUB, stride=0), :][:1]

    def gather(u):
        q, odd = u // 2, lax.rem(u, 2)

        @pl.when(u == 2)
        def _():
            for k in range(3):
                load(k, 6 + k, 0, blocks * (TILES - 1)).wait()

        summarize(q, lax.rem(1 - core + odd, 2))

        @pl.when(u == 0)
        def _():
            pl.semaphore_wait(barrier, n // pace - 1 + (pace == 2))

        @pl.when(odd == 0)
        def _():
            mate1(q).start()

            @pl.when(q >= 2)
            def _():
                scan(q - 2)

        @pl.when(odd == 1)
        def _():
            merge(q)

    loop(0, 2 * pieces, gather)
    split(0)

    def turn(u):
        q, odd = u // 2, lax.rem(u, 2)
        return q, odd, lax.rem(core + odd + (q + pieces - 1) // pieces, 2)

    def finish(u):
        q, odd, half = turn(u)
        forward(q, half, 0)
        backward(q, half, 0, True, True)

        @pl.when(u == 0)
        def _():
            scan(pieces - 2)
            scan(pieces - 1)
            mate2(0).wait_recv()

        @pl.when(u == 1)
        def _():
            mate3(0).start()

        @pl.when((1 - odd) * q >= 1)
        def _():
            mate3(q).start()

        @pl.when(u == 2)
        def _():
            spread(0)

        @pl.when(odd * q >= 1)
        def _():
            spread(q)

        @pl.when(odd == 0)
        def _():
            split(q + 1)

        @pl.when(odd == 1)
        def _():
            mate2(q + 1).wait_recv()

    def chain(u):
        q, odd, half = turn(u)
        forward(q, half, odd)
        backward(q, half, odd, True, False)

        @pl.when(odd == 0)
        def _():
            mate3(q).start()

        @pl.when(odd == 1)
        def _():
            spread(q)

    def sums(u):
        q, odd, half = turn(u)
        backward(q, half, odd, False, True)

    loop(0, 2 * pieces - 2, finish)
    loop(2 * pieces - 2, 2 * pieces, chain)
    loop(2 * pieces - 2, 2 * pieces, sums)
    lane_sums(accb, gb_ref, tokens, n_state)
    lane_sums(accc, gc_ref, tokens, n_state)

    my_tile = me // per
    my_row = my_tile // blocks
    my_half = lax.rem(lax.rem(my_tile, blocks) + 2 * blocks - 2 * my_row, 2)

    def landed(c):
        sender = 2 * c + my_half

        @pl.when(sender != me)
        def _():
            remote(out3.at[0], in3.at[c], i3s.at[0], i3r.at[c], mate).wait_recv()

    loop(0, chips, landed)
    gr_ref[...] = lax.fori_loop(
        0, chips, lambda c, total: total + in3[c], jnp.zeros((n_state, width), F32)
    )
    for q in range(pieces):
        for copy in (mate1(q), mate2(q), mate3(q)):
            copy.wait_send()
        chip_all(out1, in1, i1s, i1r, q).wait_send()
        chip_all(out2, in2, i2s, i2r, q).wait_send()
        for jj in range(TILES):
            for s in range(per):
                slot, dest = (q * TILES + jj) * per + s, owner(q, jj, s)

                @pl.when(dest != me)
                def _():
                    rate_copy(slot, dest).wait_send()


def hand_out(*refs):
    *refs, sems = refs
    count = len(refs) // 2
    copies = [pltpu.make_async_copy(refs[k], refs[count + k], sems.at[k]) for k in range(count)]
    for copy in copies:
        copy.start()
    for copy in copies:
        copy.wait()


def shards(n, inputs, step_sizes, cotangent, input_coeffs, output_coeffs, decay_rates):
    n_state, channels = decay_rates.shape
    tokens = inputs.shape[0]
    width = channels // n
    per = LANES // width
    chips = n // 2
    block = TILES * LANES
    blocks = channels // block
    pieces = blocks // 2
    r = n_state * TILES // chips
    assert r * chips == n_state * TILES and per * width == LANES
    wide = pltpu.VMEM((tokens, n_state, LANES), F32)
    rows = pltpu.VMEM((blocks, TILES, tokens + SUB, LANES), F32)
    part = pltpu.VMEM((TILES, tokens, LANES), F32)
    fold = pltpu.VMEM((2, TILES, (GROUP + 1) * SUB, LANES), F32)
    full = pltpu.VMEM((tokens, channels), jnp.bfloat16)
    small = pltpu.VMEM((n_state, tokens), F32)
    hbm = pl.BlockSpec(memory_space=pl.ANY)
    vmem = pl.BlockSpec(memory_space=pltpu.VMEM)
    sems = pltpu.SemaphoreType.DMA((pieces,))
    outs = [
        jax.ShapeDtypeStruct((tokens, channels), jnp.bfloat16),
        jax.ShapeDtypeStruct((tokens, channels), jnp.bfloat16),
        jax.ShapeDtypeStruct((n_state, tokens), F32),
        jax.ShapeDtypeStruct((n_state, tokens), F32),
        jax.ShapeDtypeStruct((n_state, width), F32),
    ]
    held = [pltpu.VMEM(o.shape, o.dtype) for o in outs]
    results = pl.pallas_call(
        partial(whole_kernel, n),
        name="whole",
        in_specs=[hbm] * 6,
        out_specs=[vmem] * 5,
        out_shape=held,
        scratch_shapes=[
            full, full, full, small, small, pltpu.VMEM((n_state, channels), F32),
            wide, wide, wide, wide, rows, rows, rows,
            pltpu.VMEM((blocks, tokens, TILES, n_state, LANES), F32),
            pltpu.VMEM((2, tokens, TILES, n_state, LANES), F32),
            fold, fold, part, part,
            pltpu.VMEM((pieces, n_state, LANES), F32),
            pltpu.VMEM((pieces, r, LANES), F32),
            pltpu.VMEM((pieces, 2, 2 * n_state + 1, block), F32),
            pltpu.VMEM((pieces, 2 * n_state + 1, block), F32),
            pltpu.VMEM((pieces, chips, 2 * r + 1, LANES), F32),
            pltpu.VMEM((pieces, chips, 2 * r + 1, LANES), F32),
            pltpu.VMEM((pieces, chips, 2 * r, LANES), F32),
            pltpu.VMEM((pieces, chips, 2 * r, LANES), F32),
            pltpu.VMEM((2 * n_state, block), F32),
            pltpu.VMEM((pieces, 2 * n_state, block), F32),
            pltpu.VMEM((pieces, 2, 2 * n_state, block), F32),
            pltpu.VMEM((pieces, 2, n_state, block), F32),
            pltpu.VMEM((pieces, n_state, block), F32),
            pltpu.VMEM((pieces * TILES * per, n_state, width), F32),
            pltpu.VMEM((chips, n_state, width), F32),
            pltpu.SemaphoreType.DMA((9,)),
            sems, sems, sems, sems, sems, sems, sems, sems, sems, sems,
            pltpu.SemaphoreType.DMA((pieces * TILES * per,)),
            pltpu.SemaphoreType.DMA((chips,)),
        ],
        compiler_params=pltpu.CompilerParams(
            collective_id=0, has_side_effects=True, vmem_limit_bytes=60 * 1024 * 1024
        ),
    )(inputs, step_sizes, cotangent, input_coeffs, output_coeffs, decay_rates)
    return pl.pallas_call(
        hand_out,
        name="hand_out",
        in_specs=[vmem] * 5,
        out_specs=[hbm] * 5,
        out_shape=outs,
        scratch_shapes=[pltpu.SemaphoreType.DMA((5,))],
    )(*[pltpu.with_memory_space_constraint(x, pltpu.VMEM) for x in results])


def solution(mesh):
    placed = (P("seq", None), P("seq", None), P("seq", None), P(None, "seq"), P(None, "seq"), P())
    return jax.shard_map(
        partial(shards, mesh.shape["seq"]),
        mesh=mesh,
        in_specs=placed,
        out_specs=(P("seq", None), P("seq", None), P(None, "seq"), P(None, "seq"), P(None, "seq")),
        check_vma=False,
    )
```

```python
from functools import partial
import math

import jax
import jax.numpy as jnp
from jax import lax
from jax.experimental import pallas as pl
from jax.experimental.pallas import tpu as pltpu
from jax.sharding import PartitionSpec as P

LANES = 128
SUB = 8
TILES = 4
GROUP = 8
SPAN = 16
STRIDE = 32
LOG2E = math.log2(math.e)
LN2 = math.log(2.0)
F32 = jnp.float32
MESH = pl.DeviceIdType.MESH


def loop(start, stop, body):
    def step(k, _):
        body(k)
        return 0

    lax.fori_loop(start, stop, step, 0)


def expand(coef_ref, wide, tokens, n_state):
    for t in range(tokens):
        wide[t] = jnp.broadcast_to(coef_ref[:, t : t + 1], (n_state, LANES))


def lane_sums(acc, out_ref, tokens, n_state):
    lane = lax.broadcasted_iota(jnp.int32, (n_state, tokens), 1)
    total = jnp.zeros((n_state, tokens), F32)
    for t in range(tokens):
        total = jnp.where(lane == t, jnp.sum(acc[t], axis=1, keepdims=True), total)
    out_ref[...] = total


def cols(jj):
    return slice(jj * LANES, (jj + 1) * LANES)


def whole_kernel(
    n,
    x_hbm, d_hbm, g_hbm, b_hbm, c_hbm, a_hbm,
    giv, gsv, gb_ref, gc_ref, gr_ref,
    xv, dv, gv, bv, cv, av,
    bx, cx, accb, accc, dl, uu, gg, dec, hs, csp, awp, cs, ws, mine, own,
    sm, rv, out1, in1, out2, in2, st2, tmp, hst, rp, rr, out3, in3,
    ins, d1s, d1r, i1s, i1r, i2s, i2r, d2s, d2r, d3s, d3r, i3s, i3r,
):
    me = lax.axis_index("seq")
    core, chip = lax.rem(me, 2), me // 2
    mate = 2 * chip + 1 - core
    tokens, channels = xv.shape
    n_state = av.shape[0]
    chips = n // 2
    blocks = channels // (LANES * TILES)
    pieces = blocks // 2
    share = chips // TILES
    r = n_state // share
    width = channels // n
    per = LANES // width
    first = core == 0
    barrier = pltpu.get_barrier_semaphore()

    coefs = [
        pltpu.make_async_copy(src, dst, ins.at[k])
        for k, (src, dst) in enumerate([(b_hbm, bv), (c_hbm, cv), (a_hbm, av)])
    ]
    bulk = [(d_hbm, dv), (x_hbm, xv), (g_hbm, gv)]
    starts = [(blocks + 2) * jj for jj in range(TILES)]

    def load(k, sem, tile, count):
        at = pl.ds(tile * LANES, count * LANES)
        src, dst = bulk[k]
        return pltpu.make_async_copy(src.at[:, at], dst.at[:, at], ins.at[sem])

    for copy in coefs:
        copy.start()
    for k in range(3):
        for tile in starts:
            load(k, 3 + k, tile, 2).start()
    for k in range(3):
        for tile in starts[:-1]:
            load(k, 6 + k, tile + 2, blocks).start()

    pace = 2 if per == 1 else 1

    def tell(dest):
        pl.semaphore_signal(barrier, inc=1, device_id=(dest,), device_id_type=MESH)

    loop(1, n // pace, lambda k: tell(lax.rem(me + pace * k, n)))
    if pace == 2:
        tell(mate)

    def tile_of(b, jj):
        return blocks * jj + lax.rem(b + 2 * jj, blocks)

    def lanes_of(b, jj):
        return pl.ds(pl.multiple_of(tile_of(b, jj) * LANES, LANES), LANES)

    def remote(src, dst, send_sem, recv_sem, dest):
        return pltpu.make_async_remote_copy(
            src_ref=src, dst_ref=dst, send_sem=send_sem, recv_sem=recv_sem,
            device_id=(dest,), device_id_type=MESH,
        )

    def row(ref, b, t):
        return ref.at[b][:, pl.ds(t, n_state, stride=0), :]

    def rates_of(b):
        return jnp.stack([av[:, lanes_of(b, jj)] * (-LOG2E) for jj in range(TILES)])

    state_shape = (TILES, n_state, LANES)
    spans = tokens // SPAN

    def summarize(q, half):
        b = 2 * q + half
        for jj in range(TILES):
            lanes = lanes_of(b, jj)
            delta = dv[:, lanes].astype(F32)
            dl[b, jj, :tokens] = delta
            uu[b, jj, :tokens] = delta * xv[:, lanes].astype(F32)
            gg[b, jj, :tokens] = gv[:, lanes].astype(F32)
            sm[q, half, 2 * n_state :, cols(jj)] = jnp.sum(delta, axis=0, keepdims=True)
        rates = rates_of(b)

        def ahead(i, end):
            for s in range(STRIDE):
                t = i * STRIDE + s
                decay = jnp.exp2(row(dl, b, t) * rates)
                dec[b, t] = decay
                end = decay * end + bx[t][None] * row(uu, b, t)
            return end

        def behind(i, back):
            for s in reversed(range(STRIDE)):
                t = tokens - STRIDE - i * STRIDE + s
                back = dec[b, t] * (cx[t][None] * row(gg, b, t) + back)
            return back

        zero = jnp.zeros(state_shape, F32)
        end = lax.fori_loop(0, tokens // STRIDE, ahead, zero)
        back = lax.fori_loop(0, tokens // STRIDE, behind, zero)
        for jj in range(TILES):
            sm[q, half, :n_state, cols(jj)] = end[jj]
            sm[q, half, n_state : 2 * n_state, cols(jj)] = back[jj]

    def mate1(q):
        return remote(sm.at[q, 1 - core], rv.at[q], d1s.at[q], d1r.at[q], mate)

    def pair_of(q, jj):
        rates = av[:, lanes_of(2 * q + core, jj)] * (-LOG2E)
        kept = sm.at[q, core]
        end_m, back_m = kept[:n_state, cols(jj)], kept[n_state : 2 * n_state, cols(jj)]
        sum_m = kept[2 * n_state :, cols(jj)]
        end_t, back_t = rv[q, :n_state, cols(jj)], rv[q, n_state : 2 * n_state, cols(jj)]
        sum_t = rv[q, 2 * n_state :, cols(jj)]
        pick = lambda a, b: (jnp.where(first, a, b), jnp.where(first, b, a))
        return rates, pick(end_m, end_t), pick(back_m, back_t), pick(sum_m, sum_t)

    def chip_copy(src, dst, send_sem, recv_sem, q, there):
        return remote(
            src.at[q, there], dst.at[q, chip], send_sem.at[q], recv_sem.at[q], 2 * there + core
        )

    def chip_sends(*refs):
        for k in range(1, chips):
            chip_copy(*refs, lax.rem(chip + k, chips)).start()

    def chip_all(src, dst, send_sem, recv_sem, q):
        part = pl.ds(0, chips - 1)
        return remote(src.at[q, part], dst.at[q, part], send_sem.at[q], recv_sem.at[q], mate)

    def merge(q):
        mate1(q).wait_recv()
        for jj in range(TILES):
            rates, (end0, end1), (back0, back1), (sum0, sum1) = pair_of(q, jj)
            end = jnp.exp2(rates * sum1) * end0 + end1
            back = back0 + jnp.exp2(rates * sum0) * back1
            for i in range(share):
                slot, rows = jj * share + i, slice(i * r, (i + 1) * r)
                out1[q, slot, :r] = end[rows]
                out1[q, slot, r : 2 * r] = back[rows]
                out1[q, slot, 2 * r :] = sum0 + sum1
        in1[q, chip] = out1[q, chip]
        chip_sends(out1, in1, i1s, i1r, q)

    def scan(q):
        chip_all(out1, in1, i1s, i1r, q).wait_recv()
        rates = own[q]

        def step(c, carry):
            ahead, behind = carry
            e = chips - 1 - c
            out2[q, c, :r] = ahead
            out2[q, e, r:] = behind
            ahead = jnp.exp2(rates * in1[q, c, 2 * r :]) * ahead + in1[q, c, :r]
            behind = jnp.exp2(rates * in1[q, e, 2 * r :]) * behind + in1[q, e, r : 2 * r]
            return ahead, behind

        blank = jnp.zeros((r, LANES), F32)
        lax.fori_loop(0, chips, step, (blank, blank), unroll=8)
        in2[q, chip] = out2[q, chip]
        chip_sends(out2, in2, i2s, i2r, q)

    def mate2(q):
        return remote(tmp.at[q], hst.at[q, core], d2s.at[q], d2r.at[q], mate)

    def split(q):
        chip_all(out2, in2, i2s, i2r, q).wait_recv()
        for jj in range(TILES):
            for i in range(share):
                slot, at = jj * share + i, i * r
                st2[at : at + r, cols(jj)] = in2[q, slot, :r]
                st2[n_state + at : n_state + at + r, cols(jj)] = in2[q, slot, r:]
        for jj in range(TILES):
            rates, (end0, _), (_, back1), (sum0, sum1) = pair_of(q, jj)
            head0, tail1 = st2[:n_state, cols(jj)], st2[n_state:, cols(jj)]
            head1 = jnp.exp2(rates * sum0) * head0 + end0
            tail0 = jnp.exp2(rates * sum1) * tail1 + back1
            hst[q, core, :n_state, cols(jj)] = jnp.where(first, head0, head1)
            hst[q, core, n_state:, cols(jj)] = jnp.where(first, tail0, tail1)
            tmp[q, :n_state, cols(jj)] = jnp.where(first, head1, head0)
            tmp[q, n_state:, cols(jj)] = jnp.where(first, tail1, tail0)
        mate2(q).start()

    def forward(q, half, slot):
        b = 2 * q + half
        held = hs.at[slot]

        def ahead(i, hidden):
            for s in range(STRIDE):
                t = i * STRIDE + s
                held[t] = hidden
                hidden = dec[b, t] * hidden + bx[t][None] * row(uu, b, t)
                accc[t] += jnp.sum(row(gg, b, t) * hidden, axis=0)
            return hidden

        start = jnp.stack([hst[q, half, :n_state, cols(jj)] for jj in range(TILES)])
        lax.fori_loop(0, tokens // STRIDE, ahead, start)

    def fold(slot, base):
        rows = pl.ds(pl.multiple_of(base, GROUP), GROUP)
        parts = [pl.ds(k * (GROUP + 1), GROUP) for k in range(SUB)]
        cs[:, rows, :] = sum(csp[slot, :, part] for part in parts)
        ws[:, rows, :] = sum(awp[slot, :, part] for part in parts)

    def backward(q, half, place, chain, sums):
        b = 2 * q + half
        held = hs.at[place]
        rates = rates_of(b)

        def halves(x):
            return sum(x[:, h : h + SUB] for h in range(0, n_state, SUB))

        def behind(i, carry):
            later, rate = carry
            base = tokens - SPAN - i * SPAN
            for slot in (1, 0):
                for s in reversed(range(GROUP)):
                    t = base + slot * GROUP + s
                    if chain:
                        state = cx[t][None] * row(gg, b, t) + later
                        later = dec[b, t] * state
                        weighted = later * held[t]
                        rate = rate + weighted * row(dl, b, t)
                    else:
                        state, weighted = dec[b, t], held[t]
                    if sums:
                        at = pl.ds(s, SUB, stride=GROUP + 1)
                        csp[slot, :, at, :] = halves(state * bx[t][None])
                        awp[slot, :, at, :] = halves(weighted * rates)
                        accb[t] += jnp.sum(state * row(uu, b, t), axis=0)
                    else:
                        dec[b, t] = state
                        held[t] = weighted
                if sums and slot:
                    fold(0, jnp.minimum(base + SPAN, tokens - GROUP))
                elif sums:
                    fold(1, base + GROUP)
            return later, rate

        last = jnp.stack([hst[q, half, n_state:, cols(jj)] for jj in range(TILES)])
        carry = (last, jnp.zeros(state_shape, F32)) if chain else (0, 0)
        _, rate = lax.fori_loop(0, spans, behind, carry)
        if chain:
            for jj in range(TILES):
                rp[q, half, :, cols(jj)] = -rate[jj]
        if sums:
            fold(0, 0)
            for jj in range(TILES):
                lanes = lanes_of(b, jj)
                giv[:, lanes] = (dl[b, jj, :tokens] * cs[jj]).astype(giv.dtype)
                x = xv[:, lanes].astype(F32)
                gsv[:, lanes] = (x * cs[jj] + LN2 * ws[jj]).astype(gsv.dtype)

    def mate3(q):
        return remote(rp.at[q, 1 - core], rr.at[q], d3s.at[q], d3r.at[q], mate)

    def owner(q, jj, s):
        return tile_of(2 * q + core, jj) * per + s

    def rate_copy(slot, dest):
        return remote(out3.at[slot], in3.at[chip], i3s.at[slot], i3r.at[chip], dest)

    def spread(q):
        mate3(q).wait_recv()
        for jj in range(TILES):
            total = rp[q, core, :, cols(jj)] + rr[q, :, cols(jj)]
            for s in range(per):
                slot, dest = (q * TILES + jj) * per + s, owner(q, jj, s)
                out3[slot] = total[:, s * width : (s + 1) * width]

                @pl.when(dest != me)
                def _():
                    rate_copy(slot, dest).start()

                @pl.when(dest == me)
                def _():
                    in3[chip] = out3[slot]

    accb[...] = jnp.zeros_like(accb)
    accc[...] = jnp.zeros_like(accc)
    csp[0] = jnp.zeros(csp.shape[1:], F32)
    awp[0] = jnp.zeros(awp.shape[1:], F32)
    coefs[0].wait()
    expand(bv, bx, tokens, n_state)
    coefs[1].wait()
    expand(cv, cx, tokens, n_state)
    coefs[2].wait()
    for k in range(3):
        load(k, 3 + k, 0, 2 * TILES).wait()
    own_tile, own_row = chip // share, lax.rem(chip, share) * r
    for q in range(pieces):
        mine[q] = av[:, lanes_of(2 * q + core, own_tile)] * (-LOG2E)
        for i in range(r):
            own[q, i : i + 1] = mine.at[q][pl.ds(own_row + i, SUB, stride=0), :][:1]

    def gather(u):
        q, odd = u // 2, lax.rem(u, 2)

        @pl.when(u == 2)
        def _():
            for k in range(3):
                load(k, 6 + k, 0, blocks * (TILES - 1)).wait()

        summarize(q, lax.rem(1 - core + odd, 2))

        @pl.when(u == 0)
        def _():
            pl.semaphore_wait(barrier, n // pace - 1 + (pace == 2))

        @pl.when(odd == 0)
        def _():
            mate1(q).start()

            @pl.when(q >= 2)
            def _():
                scan(q - 2)

        @pl.when(odd == 1)
        def _():
            merge(q)

    loop(0, 2 * pieces, gather)
    split(0)

    def turn(u):
        q, odd = u // 2, lax.rem(u, 2)
        return q, odd, lax.rem(core + odd + (q + pieces - 1) // pieces, 2)

    def finish(u):
        q, odd, half = turn(u)
        forward(q, half, 0)
        backward(q, half, 0, True, True)

        @pl.when(u == 0)
        def _():
            scan(pieces - 2)
            scan(pieces - 1)
            mate2(0).wait_recv()

        @pl.when(u == 1)
        def _():
            mate3(0).start()

        @pl.when((1 - odd) * q >= 1)
        def _():
            mate3(q).start()

        @pl.when(u == 2)
        def _():
            spread(0)

        @pl.when(odd * q >= 1)
        def _():
            spread(q)

        @pl.when(odd == 0)
        def _():
            split(q + 1)

        @pl.when(odd == 1)
        def _():
            mate2(q + 1).wait_recv()

    def chain(u):
        q, odd, half = turn(u)
        forward(q, half, odd)
        backward(q, half, odd, True, False)

        @pl.when(odd == 0)
        def _():
            mate3(q).start()

        @pl.when(odd == 1)
        def _():
            spread(q)

    def sums(u):
        q, odd, half = turn(u)
        backward(q, half, odd, False, True)

    loop(0, 2 * pieces - 2, finish)
    loop(2 * pieces - 2, 2 * pieces, chain)
    loop(2 * pieces - 2, 2 * pieces, sums)
    lane_sums(accb, gb_ref, tokens, n_state)
    lane_sums(accc, gc_ref, tokens, n_state)

    my_tile = me // per
    my_row = my_tile // blocks
    my_half = lax.rem(lax.rem(my_tile, blocks) + 2 * blocks - 2 * my_row, 2)

    def landed(c):
        sender = 2 * c + my_half

        @pl.when(sender != me)
        def _():
            remote(out3.at[0], in3.at[c], i3s.at[0], i3r.at[c], mate).wait_recv()

    loop(0, chips, landed)
    gr_ref[...] = lax.fori_loop(
        0, chips, lambda c, total: total + in3[c], jnp.zeros((n_state, width), F32)
    )
    for q in range(pieces):
        for copy in (mate1(q), mate2(q), mate3(q)):
            copy.wait_send()
        chip_all(out1, in1, i1s, i1r, q).wait_send()
        chip_all(out2, in2, i2s, i2r, q).wait_send()
        for jj in range(TILES):
            for s in range(per):
                slot, dest = (q * TILES + jj) * per + s, owner(q, jj, s)

                @pl.when(dest != me)
                def _():
                    rate_copy(slot, dest).wait_send()


def hand_out(*refs):
    *refs, sems = refs
    count = len(refs) // 2
    copies = [pltpu.make_async_copy(refs[k], refs[count + k], sems.at[k]) for k in range(count)]
    for copy in copies:
        copy.start()
    for copy in copies:
        copy.wait()


def shards(n, inputs, step_sizes, cotangent, input_coeffs, output_coeffs, decay_rates):
    n_state, channels = decay_rates.shape
    tokens = inputs.shape[0]
    width = channels // n
    per = LANES // width
    chips = n // 2
    block = TILES * LANES
    blocks = channels // block
    pieces = blocks // 2
    r = n_state * TILES // chips
    assert r * chips == n_state * TILES and per * width == LANES
    wide = pltpu.VMEM((tokens, n_state, LANES), F32)
    rows = pltpu.VMEM((blocks, TILES, tokens + SUB, LANES), F32)
    part = pltpu.VMEM((TILES, tokens, LANES), F32)
    fold = pltpu.VMEM((2, TILES, (GROUP + 1) * SUB, LANES), F32)
    full = pltpu.VMEM((tokens, channels), jnp.bfloat16)
    small = pltpu.VMEM((n_state, tokens), F32)
    hbm = pl.BlockSpec(memory_space=pl.ANY)
    vmem = pl.BlockSpec(memory_space=pltpu.VMEM)
    sems = pltpu.SemaphoreType.DMA((pieces,))
    outs = [
        jax.ShapeDtypeStruct((tokens, channels), jnp.bfloat16),
        jax.ShapeDtypeStruct((tokens, channels), jnp.bfloat16),
        jax.ShapeDtypeStruct((n_state, tokens), F32),
        jax.ShapeDtypeStruct((n_state, tokens), F32),
        jax.ShapeDtypeStruct((n_state, width), F32),
    ]
    held = [pltpu.VMEM(o.shape, o.dtype) for o in outs]
    results = pl.pallas_call(
        partial(whole_kernel, n),
        name="whole",
        in_specs=[hbm] * 6,
        out_specs=[vmem] * 5,
        out_shape=held,
        scratch_shapes=[
            full, full, full, small, small, pltpu.VMEM((n_state, channels), F32),
            wide, wide, wide, wide, rows, rows, rows,
            pltpu.VMEM((blocks, tokens, TILES, n_state, LANES), F32),
            pltpu.VMEM((2, tokens, TILES, n_state, LANES), F32),
            fold, fold, part, part,
            pltpu.VMEM((pieces, n_state, LANES), F32),
            pltpu.VMEM((pieces, r, LANES), F32),
            pltpu.VMEM((pieces, 2, 2 * n_state + 1, block), F32),
            pltpu.VMEM((pieces, 2 * n_state + 1, block), F32),
            pltpu.VMEM((pieces, chips, 2 * r + 1, LANES), F32),
            pltpu.VMEM((pieces, chips, 2 * r + 1, LANES), F32),
            pltpu.VMEM((pieces, chips, 2 * r, LANES), F32),
            pltpu.VMEM((pieces, chips, 2 * r, LANES), F32),
            pltpu.VMEM((2 * n_state, block), F32),
            pltpu.VMEM((pieces, 2 * n_state, block), F32),
            pltpu.VMEM((pieces, 2, 2 * n_state, block), F32),
            pltpu.VMEM((pieces, 2, n_state, block), F32),
            pltpu.VMEM((pieces, n_state, block), F32),
            pltpu.VMEM((pieces * TILES * per, n_state, width), F32),
            pltpu.VMEM((chips, n_state, width), F32),
            pltpu.SemaphoreType.DMA((9,)),
            sems, sems, sems, sems, sems, sems, sems, sems, sems, sems,
            pltpu.SemaphoreType.DMA((pieces * TILES * per,)),
            pltpu.SemaphoreType.DMA((chips,)),
        ],
        compiler_params=pltpu.CompilerParams(
            collective_id=0, has_side_effects=True, vmem_limit_bytes=60 * 1024 * 1024
        ),
    )(inputs, step_sizes, cotangent, input_coeffs, output_coeffs, decay_rates)
    return pl.pallas_call(
        hand_out,
        name="hand_out",
        in_specs=[vmem] * 5,
        out_specs=[hbm] * 5,
        out_shape=outs,
        scratch_shapes=[pltpu.SemaphoreType.DMA((5,))],
    )(*[pltpu.with_memory_space_constraint(x, pltpu.VMEM) for x in results])


def solution(mesh):
    placed = (P("seq", None), P("seq", None), P("seq", None), P(None, "seq"), P(None, "seq"), P())
    return jax.shard_map(
        partial(shards, mesh.shape["seq"]),
        mesh=mesh,
        in_specs=placed,
        out_specs=(P("seq", None), P("seq", None), P(None, "seq"), P(None, "seq"), P(None, "seq")),
        check_vma=False,
    )
```

```python
from functools import partial
import math

import jax
import jax.numpy as jnp
from jax import lax
from jax.experimental import pallas as pl
from jax.experimental.pallas import tpu as pltpu
from jax.sharding import PartitionSpec as P

LANES = 128
SUB = 8
TILES = 4
GROUP = 8
SPAN = 16
STRIDE = 32
LOG2E = math.log2(math.e)
LN2 = math.log(2.0)
F32 = jnp.float32
MESH = pl.DeviceIdType.MESH


def loop(start, stop, body):
    def step(k, _):
        body(k)
        return 0

    lax.fori_loop(start, stop, step, 0)


def expand(coef_ref, wide, tokens, n_state):
    for t in range(tokens):
        wide[t] = jnp.broadcast_to(coef_ref[:, t : t + 1], (n_state, LANES))


def lane_sums(acc, out_ref, tokens, n_state):
    lane = lax.broadcasted_iota(jnp.int32, (n_state, tokens), 1)
    total = jnp.zeros((n_state, tokens), F32)
    for t in range(tokens):
        total = jnp.where(lane == t, jnp.sum(acc[t], axis=1, keepdims=True), total)
    out_ref[...] = total


def cols(jj):
    return slice(jj * LANES, (jj + 1) * LANES)


def whole_kernel(
    n,
    x_hbm, d_hbm, g_hbm, b_hbm, c_hbm, a_hbm,
    giv, gsv, accb, accc, gr_ref,
    xv, dv, gv, bv, cv, av,
    bx, cx, dl, uu, gg, dec, hs, csp, awp, cs, ws, mine, own,
    sm, rv, out1, in1, out2, in2, st2, tmp, hst, rp, rr, out3, in3,
    ins, d1s, d1r, i1s, i1r, i2s, i2r, d2s, d2r, d3s, d3r, i3s, i3r,
):
    me = lax.axis_index("seq")
    core, chip = lax.rem(me, 2), me // 2
    mate = 2 * chip + 1 - core
    tokens, channels = xv.shape
    n_state = av.shape[0]
    chips = n // 2
    blocks = channels // (LANES * TILES)
    pieces = blocks // 2
    share = chips // TILES
    r = n_state // share
    width = channels // n
    per = LANES // width
    first = core == 0
    barrier = pltpu.get_barrier_semaphore()

    coefs = [
        pltpu.make_async_copy(src, dst, ins.at[k])
        for k, (src, dst) in enumerate([(b_hbm, bv), (c_hbm, cv), (a_hbm, av)])
    ]
    bulk = [(d_hbm, dv), (x_hbm, xv), (g_hbm, gv)]
    starts = [(blocks + 2) * jj for jj in range(TILES)]

    def load(k, sem, tile, count):
        at = pl.ds(tile * LANES, count * LANES)
        src, dst = bulk[k]
        return pltpu.make_async_copy(src.at[:, at], dst.at[:, at], ins.at[sem])

    for copy in coefs:
        copy.start()
    for k in range(3):
        for tile in starts:
            load(k, 3 + k, tile, 2).start()
    for k in range(3):
        for tile in starts[:-1]:
            load(k, 6 + k, tile + 2, blocks).start()

    pace = 2 if per == 1 else 1

    def tell(dest):
        pl.semaphore_signal(barrier, inc=1, device_id=(dest,), device_id_type=MESH)

    for k in range(1, n // pace):
        tell(lax.rem(me + pace * k, n))
    if pace == 2:
        tell(mate)

    def tile_of(b, jj):
        return blocks * jj + lax.rem(b + 2 * jj, blocks)

    def lanes_of(b, jj):
        return pl.ds(pl.multiple_of(tile_of(b, jj) * LANES, LANES), LANES)

    def remote(src, dst, send_sem, recv_sem, dest):
        return pltpu.make_async_remote_copy(
            src_ref=src, dst_ref=dst, send_sem=send_sem, recv_sem=recv_sem,
            device_id=(dest,), device_id_type=MESH,
        )

    def row(ref, b, t):
        return ref.at[b][:, pl.ds(t, n_state, stride=0), :]

    def rates_of(b):
        return jnp.stack([av[:, lanes_of(b, jj)] * (-LOG2E) for jj in range(TILES)])

    state_shape = (TILES, n_state, LANES)
    spans = tokens // SPAN

    def summarize(q, half):
        b = 2 * q + half
        for jj in range(TILES):
            lanes = lanes_of(b, jj)
            delta = dv[:, lanes].astype(F32)
            dl[b, jj, :tokens] = delta
            uu[b, jj, :tokens] = delta * xv[:, lanes].astype(F32)
            gg[b, jj, :tokens] = gv[:, lanes].astype(F32)
            sm[q, half, 2 * n_state :, cols(jj)] = jnp.sum(delta, axis=0, keepdims=True)
        rates = rates_of(b)

        def ahead(i, end):
            for s in range(STRIDE):
                t = i * STRIDE + s
                decay = jnp.exp2(row(dl, b, t) * rates)
                dec[b, t] = decay
                end = decay * end + bx[t][None] * row(uu, b, t)
            return end

        def behind(i, back):
            for s in reversed(range(STRIDE)):
                t = tokens - STRIDE - i * STRIDE + s
                back = dec[b, t] * (cx[t][None] * row(gg, b, t) + back)
            return back

        zero = jnp.zeros(state_shape, F32)
        end = lax.fori_loop(0, tokens // STRIDE, ahead, zero)
        back = lax.fori_loop(0, tokens // STRIDE, behind, zero)
        for jj in range(TILES):
            sm[q, half, :n_state, cols(jj)] = end[jj]
            sm[q, half, n_state : 2 * n_state, cols(jj)] = back[jj]

    def mate1(q):
        return remote(sm.at[q, 1 - core], rv.at[q], d1s.at[q], d1r.at[q], mate)

    def pair_of(q, jj):
        rates = av[:, lanes_of(2 * q + core, jj)] * (-LOG2E)
        kept = sm.at[q, core]
        end_m, back_m = kept[:n_state, cols(jj)], kept[n_state : 2 * n_state, cols(jj)]
        sum_m = kept[2 * n_state :, cols(jj)]
        end_t, back_t = rv[q, :n_state, cols(jj)], rv[q, n_state : 2 * n_state, cols(jj)]
        sum_t = rv[q, 2 * n_state :, cols(jj)]
        pick = lambda a, b: (jnp.where(first, a, b), jnp.where(first, b, a))
        return rates, pick(end_m, end_t), pick(back_m, back_t), pick(sum_m, sum_t)

    def chip_copy(src, dst, send_sem, recv_sem, q, there):
        return remote(
            src.at[q, there], dst.at[q, chip], send_sem.at[q], recv_sem.at[q], 2 * there + core
        )

    def chip_sends(*refs):
        for k in range(1, chips):
            chip_copy(*refs, lax.rem(chip + k, chips)).start()

    def chip_all(src, dst, send_sem, recv_sem, q):
        part = pl.ds(0, chips - 1)
        return remote(src.at[q, part], dst.at[q, part], send_sem.at[q], recv_sem.at[q], mate)

    def merge(q):
        mate1(q).wait_recv()
        for jj in range(TILES):
            rates, (end0, end1), (back0, back1), (sum0, sum1) = pair_of(q, jj)
            end = jnp.exp2(rates * sum1) * end0 + end1
            back = back0 + jnp.exp2(rates * sum0) * back1
            for i in range(share):
                slot, rows = jj * share + i, slice(i * r, (i + 1) * r)
                out1[q, slot, :r] = end[rows]
                out1[q, slot, r : 2 * r] = back[rows]
                out1[q, slot, 2 * r :] = sum0 + sum1
        in1[q, chip] = out1[q, chip]
        chip_sends(out1, in1, i1s, i1r, q)

    def scan(q):
        chip_all(out1, in1, i1s, i1r, q).wait_recv()
        rates = own[q]

        def step(c, carry):
            ahead, behind = carry
            e = chips - 1 - c
            out2[q, c, :r] = ahead
            out2[q, e, r:] = behind
            ahead = jnp.exp2(rates * in1[q, c, 2 * r :]) * ahead + in1[q, c, :r]
            behind = jnp.exp2(rates * in1[q, e, 2 * r :]) * behind + in1[q, e, r : 2 * r]
            return ahead, behind

        blank = jnp.zeros((r, LANES), F32)
        lax.fori_loop(0, chips, step, (blank, blank), unroll=8)
        in2[q, chip] = out2[q, chip]
        chip_sends(out2, in2, i2s, i2r, q)

    def mate2(q):
        return remote(tmp.at[q], hst.at[q, core], d2s.at[q], d2r.at[q], mate)

    def split(q):
        chip_all(out2, in2, i2s, i2r, q).wait_recv()
        for jj in range(TILES):
            for i in range(share):
                slot, at = jj * share + i, i * r
                st2[at : at + r, cols(jj)] = in2[q, slot, :r]
                st2[n_state + at : n_state + at + r, cols(jj)] = in2[q, slot, r:]
        for jj in range(TILES):
            rates, (end0, _), (_, back1), (sum0, sum1) = pair_of(q, jj)
            head0, tail1 = st2[:n_state, cols(jj)], st2[n_state:, cols(jj)]
            head1 = jnp.exp2(rates * sum0) * head0 + end0
            tail0 = jnp.exp2(rates * sum1) * tail1 + back1
            hst[q, core, :n_state, cols(jj)] = jnp.where(first, head0, head1)
            hst[q, core, n_state:, cols(jj)] = jnp.where(first, tail0, tail1)
            tmp[q, :n_state, cols(jj)] = jnp.where(first, head1, head0)
            tmp[q, n_state:, cols(jj)] = jnp.where(first, tail1, tail0)
        mate2(q).start()

    def forward(q, half, slot):
        b = 2 * q + half
        held = hs.at[slot]

        def ahead(i, hidden):
            for s in range(STRIDE):
                t = i * STRIDE + s
                held[t] = hidden
                hidden = dec[b, t] * hidden + bx[t][None] * row(uu, b, t)
                accc[t] += jnp.sum(row(gg, b, t) * hidden, axis=0)
            return hidden

        start = jnp.stack([hst[q, half, :n_state, cols(jj)] for jj in range(TILES)])
        lax.fori_loop(0, tokens // STRIDE, ahead, start)

    def fold(slot, base):
        rows = pl.ds(pl.multiple_of(base, GROUP), GROUP)
        parts = [pl.ds(k * (GROUP + 1), GROUP) for k in range(SUB)]
        cs[:, rows, :] = sum(csp[slot, :, part] for part in parts)
        ws[:, rows, :] = sum(awp[slot, :, part] for part in parts)

    def backward(q, half, place, chain, sums):
        b = 2 * q + half
        held = hs.at[place]
        rates = rates_of(b)

        def halves(x):
            return sum(x[:, h : h + SUB] for h in range(0, n_state, SUB))

        def behind(i, carry):
            later, rate = carry
            base = tokens - SPAN - i * SPAN
            for slot in (1, 0):
                for s in reversed(range(GROUP)):
                    t = base + slot * GROUP + s
                    if chain:
                        state = cx[t][None] * row(gg, b, t) + later
                        later = dec[b, t] * state
                        weighted = later * held[t]
                        rate = rate + weighted * row(dl, b, t)
                    else:
                        state, weighted = dec[b, t], held[t]
                    if sums:
                        at = pl.ds(s, SUB, stride=GROUP + 1)
                        csp[slot, :, at, :] = halves(state * bx[t][None])
                        awp[slot, :, at, :] = halves(weighted * rates)
                        accb[t] += jnp.sum(state * row(uu, b, t), axis=0)
                    else:
                        dec[b, t] = state
                        held[t] = weighted
                if sums and slot:
                    fold(0, jnp.minimum(base + SPAN, tokens - GROUP))
                elif sums:
                    fold(1, base + GROUP)
            return later, rate

        last = jnp.stack([hst[q, half, n_state:, cols(jj)] for jj in range(TILES)])
        carry = (last, jnp.zeros(state_shape, F32)) if chain else (0, 0)
        _, rate = lax.fori_loop(0, spans, behind, carry)
        if chain:
            for jj in range(TILES):
                rp[q, half, :, cols(jj)] = -rate[jj]
        if sums:
            fold(0, 0)
            for jj in range(TILES):
                lanes = lanes_of(b, jj)
                giv[:, lanes] = (dl[b, jj, :tokens] * cs[jj]).astype(giv.dtype)
                x = xv[:, lanes].astype(F32)
                gsv[:, lanes] = (x * cs[jj] + LN2 * ws[jj]).astype(gsv.dtype)

    def mate3(q):
        return remote(rp.at[q, 1 - core], rr.at[q], d3s.at[q], d3r.at[q], mate)

    def owner(q, jj, s):
        return tile_of(2 * q + core, jj) * per + s

    def rate_copy(slot, dest):
        return remote(out3.at[slot], in3.at[chip], i3s.at[slot], i3r.at[chip], dest)

    def spread(q):
        mate3(q).wait_recv()
        for jj in range(TILES):
            total = rp[q, core, :, cols(jj)] + rr[q, :, cols(jj)]
            for s in range(per):
                slot, dest = (q * TILES + jj) * per + s, owner(q, jj, s)
                out3[slot] = total[:, s * width : (s + 1) * width]

                @pl.when(dest != me)
                def _():
                    rate_copy(slot, dest).start()

                @pl.when(dest == me)
                def _():
                    in3[chip] = out3[slot]

    accb[...] = jnp.zeros_like(accb)
    accc[...] = jnp.zeros_like(accc)
    csp[0] = jnp.zeros(csp.shape[1:], F32)
    awp[0] = jnp.zeros(awp.shape[1:], F32)
    coefs[0].wait()
    expand(bv, bx, tokens, n_state)
    coefs[1].wait()
    expand(cv, cx, tokens, n_state)
    coefs[2].wait()
    for k in range(3):
        load(k, 3 + k, 0, 2 * TILES).wait()
    own_tile, own_row = chip // share, lax.rem(chip, share) * r
    for q in range(pieces):
        mine[q] = av[:, lanes_of(2 * q + core, own_tile)] * (-LOG2E)
        for i in range(r):
            own[q, i : i + 1] = mine.at[q][pl.ds(own_row + i, SUB, stride=0), :][:1]

    def gather(u):
        q, odd = u // 2, lax.rem(u, 2)

        @pl.when(u == 2)
        def _():
            for k in range(3):
                load(k, 6 + k, 0, blocks * (TILES - 1)).wait()

        summarize(q, lax.rem(1 - core + odd, 2))

        @pl.when(u == 0)
        def _():
            pl.semaphore_wait(barrier, n // pace - 1 + (pace == 2))

        @pl.when(odd == 0)
        def _():
            mate1(q).start()

            @pl.when(q >= 2)
            def _():
                scan(q - 2)

        @pl.when(odd == 1)
        def _():
            merge(q)

    loop(0, 2 * pieces, gather)
    split(0)

    def turn(u):
        q, odd = u // 2, lax.rem(u, 2)
        return q, odd, lax.rem(core + odd + (q + pieces - 1) // pieces, 2)

    def finish(u):
        q, odd, half = turn(u)
        forward(q, half, 0)
        backward(q, half, 0, True, True)

        @pl.when(u == 0)
        def _():
            scan(pieces - 2)
            scan(pieces - 1)
            mate2(0).wait_recv()

        @pl.when(u == 1)
        def _():
            mate3(0).start()

        @pl.when((1 - odd) * q >= 1)
        def _():
            mate3(q).start()

        @pl.when(u == 2)
        def _():
            spread(0)

        @pl.when(odd * q >= 1)
        def _():
            spread(q)

        @pl.when(odd == 0)
        def _():
            split(q + 1)

        @pl.when(odd == 1)
        def _():
            mate2(q + 1).wait_recv()

    def chain(u):
        q, odd, half = turn(u)
        forward(q, half, odd)
        backward(q, half, odd, True, False)

        @pl.when(odd == 0)
        def _():
            mate3(q).start()

        @pl.when(odd == 1)
        def _():
            spread(q)

    def sums(u):
        q, odd, half = turn(u)
        backward(q, half, odd, False, True)

    loop(0, 2 * pieces - 2, finish)
    loop(2 * pieces - 2, 2 * pieces, chain)
    loop(2 * pieces - 2, 2 * pieces, sums)

    my_tile = me // per
    my_row = my_tile // blocks
    my_half = lax.rem(lax.rem(my_tile, blocks) + 2 * blocks - 2 * my_row, 2)

    def landed(c):
        sender = 2 * c + my_half

        @pl.when(sender != me)
        def _():
            remote(out3.at[0], in3.at[c], i3s.at[0], i3r.at[c], mate).wait_recv()

    loop(0, chips, landed)
    gr_ref[...] = lax.fori_loop(
        0, chips, lambda c, total: total + in3[c], jnp.zeros((n_state, width), F32)
    )
    for q in range(pieces):
        for copy in (mate1(q), mate2(q), mate3(q)):
            copy.wait_send()
        chip_all(out1, in1, i1s, i1r, q).wait_send()
        chip_all(out2, in2, i2s, i2r, q).wait_send()
        for jj in range(TILES):
            for s in range(per):
                slot, dest = (q * TILES + jj) * per + s, owner(q, jj, s)

                @pl.when(dest != me)
                def _():
                    rate_copy(slot, dest).wait_send()


def hand_out(
    giv, gsv, accb, accc, gr_ref, gi_hbm, gs_hbm, gb_hbm, gc_hbm, gr_hbm, gb_ref, gc_ref, sems
):
    tokens, n_state = accb.shape[:2]
    pairs = [(giv, gi_hbm), (gsv, gs_hbm), (gr_ref, gr_hbm), (gb_ref, gb_hbm), (gc_ref, gc_hbm)]
    copies = [pltpu.make_async_copy(src, dst, sems.at[k]) for k, (src, dst) in enumerate(pairs)]
    for copy in copies[:3]:
        copy.start()
    lane_sums(accb, gb_ref, tokens, n_state)
    copies[3].start()
    lane_sums(accc, gc_ref, tokens, n_state)
    copies[4].start()
    for copy in copies:
        copy.wait()


def shards(n, inputs, step_sizes, cotangent, input_coeffs, output_coeffs, decay_rates):
    n_state, channels = decay_rates.shape
    tokens = inputs.shape[0]
    width = channels // n
    per = LANES // width
    chips = n // 2
    block = TILES * LANES
    blocks = channels // block
    pieces = blocks // 2
    r = n_state * TILES // chips
    assert r * chips == n_state * TILES and per * width == LANES
    wide = pltpu.VMEM((tokens, n_state, LANES), F32)
    rows = pltpu.VMEM((blocks, TILES, tokens + SUB, LANES), F32)
    part = pltpu.VMEM((TILES, tokens, LANES), F32)
    fold = pltpu.VMEM((2, TILES, (GROUP + 1) * SUB, LANES), F32)
    full = pltpu.VMEM((tokens, channels), jnp.bfloat16)
    small = pltpu.VMEM((n_state, tokens), F32)
    hbm = pl.BlockSpec(memory_space=pl.ANY)
    vmem = pl.BlockSpec(memory_space=pltpu.VMEM)
    sems = pltpu.SemaphoreType.DMA((pieces,))
    outs = [
        jax.ShapeDtypeStruct((tokens, channels), jnp.bfloat16),
        jax.ShapeDtypeStruct((tokens, channels), jnp.bfloat16),
        jax.ShapeDtypeStruct((n_state, tokens), F32),
        jax.ShapeDtypeStruct((n_state, tokens), F32),
        jax.ShapeDtypeStruct((n_state, width), F32),
    ]
    held = [pltpu.VMEM(o.shape, o.dtype) for o in outs]
    held[2:4] = [wide, wide]
    results = pl.pallas_call(
        partial(whole_kernel, n),
        name="whole",
        in_specs=[hbm] * 6,
        out_specs=[vmem] * 5,
        out_shape=held,
        scratch_shapes=[
            full, full, full, small, small, pltpu.VMEM((n_state, channels), F32),
            wide, wide, rows, rows, rows,
            pltpu.VMEM((blocks, tokens, TILES, n_state, LANES), F32),
            pltpu.VMEM((2, tokens, TILES, n_state, LANES), F32),
            fold, fold, part, part,
            pltpu.VMEM((pieces, n_state, LANES), F32),
            pltpu.VMEM((pieces, r, LANES), F32),
            pltpu.VMEM((pieces, 2, 2 * n_state + 1, block), F32),
            pltpu.VMEM((pieces, 2 * n_state + 1, block), F32),
            pltpu.VMEM((pieces, chips, 2 * r + 1, LANES), F32),
            pltpu.VMEM((pieces, chips, 2 * r + 1, LANES), F32),
            pltpu.VMEM((pieces, chips, 2 * r, LANES), F32),
            pltpu.VMEM((pieces, chips, 2 * r, LANES), F32),
            pltpu.VMEM((2 * n_state, block), F32),
            pltpu.VMEM((pieces, 2 * n_state, block), F32),
            pltpu.VMEM((pieces, 2, 2 * n_state, block), F32),
            pltpu.VMEM((pieces, 2, n_state, block), F32),
            pltpu.VMEM((pieces, n_state, block), F32),
            pltpu.VMEM((pieces * TILES * per, n_state, width), F32),
            pltpu.VMEM((chips, n_state, width), F32),
            pltpu.SemaphoreType.DMA((9,)),
            sems, sems, sems, sems, sems, sems, sems, sems, sems, sems,
            pltpu.SemaphoreType.DMA((pieces * TILES * per,)),
            pltpu.SemaphoreType.DMA((chips,)),
        ],
        compiler_params=pltpu.CompilerParams(
            collective_id=0, has_side_effects=True, vmem_limit_bytes=58 * 1024 * 1024
        ),
    )(inputs, step_sizes, cotangent, input_coeffs, output_coeffs, decay_rates)
    return pl.pallas_call(
        hand_out,
        name="hand_out",
        in_specs=[vmem] * 5,
        out_specs=[hbm] * 5,
        out_shape=outs,
        scratch_shapes=[small, small, pltpu.SemaphoreType.DMA((5,))],
        compiler_params=pltpu.CompilerParams(vmem_limit_bytes=8 * 1024 * 1024),
    )(*[pltpu.with_memory_space_constraint(x, pltpu.VMEM) for x in results])


def solution(mesh):
    placed = (P("seq", None), P("seq", None), P("seq", None), P(None, "seq"), P(None, "seq"), P())
    return jax.shard_map(
        partial(shards, mesh.shape["seq"]),
        mesh=mesh,
        in_specs=placed,
        out_specs=(P("seq", None), P("seq", None), P(None, "seq"), P(None, "seq"), P(None, "seq")),
        check_vma=False,
    )
```

```python
from functools import partial
import math

import jax
import jax.numpy as jnp
from jax import lax
from jax.experimental import pallas as pl
from jax.experimental.pallas import tpu as pltpu
from jax.sharding import PartitionSpec as P

LANES = 128
SUB = 8
TILES = 4
GROUP = 8
SPAN = 16
STRIDE = 32
LOG2E = math.log2(math.e)
LN2 = math.log(2.0)
F32 = jnp.float32
MESH = pl.DeviceIdType.MESH


def loop(start, stop, body):
    def step(k, _):
        body(k)
        return 0

    lax.fori_loop(start, stop, step, 0)


def expand(coef_ref, wide, tokens, n_state):
    for t in range(tokens):
        wide[t] = jnp.broadcast_to(coef_ref[:, t : t + 1], (n_state, LANES))


def lane_sums(acc, out_ref, tokens, n_state):
    lane = lax.broadcasted_iota(jnp.int32, (n_state, tokens), 1)
    total = jnp.zeros((n_state, tokens), F32)
    for t in range(tokens):
        total = jnp.where(lane == t, jnp.sum(acc[t], axis=1, keepdims=True), total)
    out_ref[...] = total


def cols(jj):
    return slice(jj * LANES, (jj + 1) * LANES)


def whole_kernel(
    n,
    x_hbm, d_hbm, g_hbm, b_hbm, c_hbm, a_hbm,
    giv, gsv, accb, accc, gr_ref,
    xv, dv, gv, bv, cv, av,
    bx, cx, dl, uu, gg, dec, hs, csp, awp, cs, ws, mine, own,
    sm, rv, out1, in1, out2, in2, st2, tmp, hst, rp, rr, out3, in3,
    ins, d1s, d1r, i1s, i1r, i2s, i2r, d2s, d2r, d3s, d3r, i3s, i3r,
):
    me = lax.axis_index("seq")
    core, chip = lax.rem(me, 2), me // 2
    mate = 2 * chip + 1 - core
    tokens, channels = xv.shape
    n_state = av.shape[0]
    chips = n // 2
    blocks = channels // (LANES * TILES)
    pieces = blocks // 2
    share = chips // TILES
    r = n_state // share
    width = channels // n
    per = LANES // width
    first = core == 0
    barrier = pltpu.get_barrier_semaphore()

    coefs = [
        pltpu.make_async_copy(src, dst, ins.at[k])
        for k, (src, dst) in enumerate([(b_hbm, bv), (c_hbm, cv), (a_hbm, av)])
    ]
    bulk = [(d_hbm, dv), (x_hbm, xv), (g_hbm, gv)]
    starts = [(blocks + 2) * jj for jj in range(TILES)]

    def load(k, sem, tile, count):
        at = pl.ds(tile * LANES, count * LANES)
        src, dst = bulk[k]
        return pltpu.make_async_copy(src.at[:, at], dst.at[:, at], ins.at[sem])

    for copy in coefs:
        copy.start()
    for k in range(3):
        for tile in starts:
            load(k, 3 + k, tile, 2).start()
    for k in range(3):
        for tile in starts[:-1]:
            load(k, 6 + k, tile + 2, blocks).start()

    pace = 2 if per == 1 else 1

    def tell(dest):
        pl.semaphore_signal(barrier, inc=1, device_id=(dest,), device_id_type=MESH)

    for k in range(1, n // pace):
        tell(lax.rem(me + pace * k, n))
    if pace == 2:
        tell(mate)

    def tile_of(b, jj):
        return blocks * jj + lax.rem(b + 2 * jj, blocks)

    def lanes_of(b, jj):
        return pl.ds(pl.multiple_of(tile_of(b, jj) * LANES, LANES), LANES)

    def remote(src, dst, send_sem, recv_sem, dest):
        return pltpu.make_async_remote_copy(
            src_ref=src, dst_ref=dst, send_sem=send_sem, recv_sem=recv_sem,
            device_id=(dest,), device_id_type=MESH,
        )

    def row(ref, b, t):
        return ref.at[b][:, pl.ds(t, n_state, stride=0), :]

    def rates_of(b):
        return jnp.stack([av[:, lanes_of(b, jj)] * (-LOG2E) for jj in range(TILES)])

    state_shape = (TILES, n_state, LANES)
    spans = tokens // SPAN

    def summarize(q, half):
        b = 2 * q + half
        for jj in range(TILES):
            lanes = lanes_of(b, jj)
            delta = dv[:, lanes].astype(F32)
            dl[b, jj, :tokens] = delta
            uu[b, jj, :tokens] = delta * xv[:, lanes].astype(F32)
            gg[b, jj, :tokens] = gv[:, lanes].astype(F32)
            sm[q, half, 2 * n_state :, cols(jj)] = jnp.sum(delta, axis=0, keepdims=True)
        rates = rates_of(b)

        def ahead(i, end):
            for s in range(STRIDE):
                t = i * STRIDE + s
                decay = jnp.exp2(row(dl, b, t) * rates)
                dec[b, t] = decay
                end = decay * end + bx[t][None] * row(uu, b, t)
            return end

        def behind(i, back):
            for s in reversed(range(STRIDE)):
                t = tokens - STRIDE - i * STRIDE + s
                back = dec[b, t] * (cx[t][None] * row(gg, b, t) + back)
            return back

        zero = jnp.zeros(state_shape, F32)
        end = lax.fori_loop(0, tokens // STRIDE, ahead, zero)
        back = lax.fori_loop(0, tokens // STRIDE, behind, zero)
        for jj in range(TILES):
            sm[q, half, :n_state, cols(jj)] = end[jj]
            sm[q, half, n_state : 2 * n_state, cols(jj)] = back[jj]

    def mate1(q):
        return remote(sm.at[q, 1 - core], rv.at[q], d1s.at[q], d1r.at[q], mate)

    def pair_of(q, jj):
        rates = av[:, lanes_of(2 * q + core, jj)] * (-LOG2E)
        kept = sm.at[q, core]
        end_m, back_m = kept[:n_state, cols(jj)], kept[n_state : 2 * n_state, cols(jj)]
        sum_m = kept[2 * n_state :, cols(jj)]
        end_t, back_t = rv[q, :n_state, cols(jj)], rv[q, n_state : 2 * n_state, cols(jj)]
        sum_t = rv[q, 2 * n_state :, cols(jj)]
        pick = lambda a, b: (jnp.where(first, a, b), jnp.where(first, b, a))
        return rates, pick(end_m, end_t), pick(back_m, back_t), pick(sum_m, sum_t)

    def chip_copy(src, dst, send_sem, recv_sem, q, there):
        return remote(
            src.at[q, there], dst.at[q, chip], send_sem.at[q], recv_sem.at[q], 2 * there + core
        )

    def chip_sends(*refs):
        for k in range(1, chips):
            chip_copy(*refs, lax.rem(chip + k, chips)).start()

    def chip_all(src, dst, send_sem, recv_sem, q):
        part = pl.ds(0, chips - 1)
        return remote(src.at[q, part], dst.at[q, part], send_sem.at[q], recv_sem.at[q], mate)

    def merge(q):
        mate1(q).wait_recv()
        for jj in range(TILES):
            rates, (end0, end1), (back0, back1), (sum0, sum1) = pair_of(q, jj)
            end = jnp.exp2(rates * sum1) * end0 + end1
            back = back0 + jnp.exp2(rates * sum0) * back1
            for i in range(share):
                slot, rows = jj * share + i, slice(i * r, (i + 1) * r)
                out1[q, slot, :r] = end[rows]
                out1[q, slot, r : 2 * r] = back[rows]
                out1[q, slot, 2 * r :] = sum0 + sum1
        in1[q, chip] = out1[q, chip]
        chip_sends(out1, in1, i1s, i1r, q)

    def scan(q):
        chip_all(out1, in1, i1s, i1r, q).wait_recv()
        rates = own[q]

        def step(c, carry):
            ahead, behind = carry
            e = chips - 1 - c
            out2[q, c, :r] = ahead
            out2[q, e, r:] = behind
            ahead = jnp.exp2(rates * in1[q, c, 2 * r :]) * ahead + in1[q, c, :r]
            behind = jnp.exp2(rates * in1[q, e, 2 * r :]) * behind + in1[q, e, r : 2 * r]
            return ahead, behind

        blank = jnp.zeros((r, LANES), F32)
        lax.fori_loop(0, chips, step, (blank, blank), unroll=8)
        in2[q, chip] = out2[q, chip]
        chip_sends(out2, in2, i2s, i2r, q)

    def mate2(q):
        return remote(tmp.at[q], hst.at[q, core], d2s.at[q], d2r.at[q], mate)

    def split(q):
        chip_all(out2, in2, i2s, i2r, q).wait_recv()
        for jj in range(TILES):
            for i in range(share):
                slot, at = jj * share + i, i * r
                st2[at : at + r, cols(jj)] = in2[q, slot, :r]
                st2[n_state + at : n_state + at + r, cols(jj)] = in2[q, slot, r:]
        for jj in range(TILES):
            rates, (end0, _), (_, back1), (sum0, sum1) = pair_of(q, jj)
            head0, tail1 = st2[:n_state, cols(jj)], st2[n_state:, cols(jj)]
            head1 = jnp.exp2(rates * sum0) * head0 + end0
            tail0 = jnp.exp2(rates * sum1) * tail1 + back1
            hst[q, core, :n_state, cols(jj)] = jnp.where(first, head0, head1)
            hst[q, core, n_state:, cols(jj)] = jnp.where(first, tail0, tail1)
            tmp[q, :n_state, cols(jj)] = jnp.where(first, head1, head0)
            tmp[q, n_state:, cols(jj)] = jnp.where(first, tail1, tail0)
        mate2(q).start()

    def forward(q, half, slot):
        b = 2 * q + half
        held = hs.at[slot]

        def ahead(i, hidden):
            for s in range(STRIDE):
                t = i * STRIDE + s
                held[t] = hidden
                hidden = dec[b, t] * hidden + bx[t][None] * row(uu, b, t)
                accc[t] += jnp.sum(row(gg, b, t) * hidden, axis=0)
            return hidden

        start = jnp.stack([hst[q, half, :n_state, cols(jj)] for jj in range(TILES)])
        lax.fori_loop(0, tokens // STRIDE, ahead, start)

    def fold(slot, base):
        rows = pl.ds(pl.multiple_of(base, GROUP), GROUP)
        parts = [pl.ds(k * (GROUP + 1), GROUP) for k in range(SUB)]
        cs[:, rows, :] = sum(csp[slot, :, part] for part in parts)
        ws[:, rows, :] = sum(awp[slot, :, part] for part in parts)

    def backward(q, half, place, chain, sums):
        b = 2 * q + half
        held = hs.at[place]
        rates = rates_of(b)

        def halves(x):
            return sum(x[:, h : h + SUB] for h in range(0, n_state, SUB))

        def behind(i, carry):
            later, rate = carry
            base = tokens - SPAN - i * SPAN
            for slot in (1, 0):
                for s in reversed(range(GROUP)):
                    t = base + slot * GROUP + s
                    if chain:
                        state = cx[t][None] * row(gg, b, t) + later
                        later = dec[b, t] * state
                        weighted = later * held[t]
                        rate = rate + weighted * row(dl, b, t)
                    else:
                        state, weighted = dec[b, t], held[t]
                    if sums:
                        at = pl.ds(s, SUB, stride=GROUP + 1)
                        csp[slot, :, at, :] = halves(state * bx[t][None])
                        awp[slot, :, at, :] = halves(weighted * rates)
                        accb[t] += jnp.sum(state * row(uu, b, t), axis=0)
                    else:
                        dec[b, t] = state
                        held[t] = weighted
                if sums and slot:
                    fold(0, jnp.minimum(base + SPAN, tokens - GROUP))
                elif sums:
                    fold(1, base + GROUP)
            return later, rate

        last = jnp.stack([hst[q, half, n_state:, cols(jj)] for jj in range(TILES)])
        carry = (last, jnp.zeros(state_shape, F32)) if chain else (0, 0)
        _, rate = lax.fori_loop(0, spans, behind, carry)
        if chain:
            for jj in range(TILES):
                rp[q, half, :, cols(jj)] = -rate[jj]
        if sums:
            fold(0, 0)
            for jj in range(TILES):
                lanes = lanes_of(b, jj)
                giv[:, lanes] = (dl[b, jj, :tokens] * cs[jj]).astype(giv.dtype)
                x = xv[:, lanes].astype(F32)
                gsv[:, lanes] = (x * cs[jj] + LN2 * ws[jj]).astype(gsv.dtype)

    def mate3(q):
        return remote(rp.at[q, 1 - core], rr.at[q], d3s.at[q], d3r.at[q], mate)

    def owner(q, jj, s):
        return tile_of(2 * q + core, jj) * per + s

    def rate_copy(slot, dest):
        return remote(out3.at[slot], in3.at[chip], i3s.at[slot], i3r.at[chip], dest)

    def spread(q):
        mate3(q).wait_recv()
        for jj in range(TILES):
            total = rp[q, core, :, cols(jj)] + rr[q, :, cols(jj)]
            for s in range(per):
                slot, dest = (q * TILES + jj) * per + s, owner(q, jj, s)
                out3[slot] = total[:, s * width : (s + 1) * width]

                @pl.when(dest != me)
                def _():
                    rate_copy(slot, dest).start()

                @pl.when(dest == me)
                def _():
                    in3[chip] = out3[slot]

    accb[...] = jnp.zeros_like(accb)
    accc[...] = jnp.zeros_like(accc)
    csp[0] = jnp.zeros(csp.shape[1:], F32)
    awp[0] = jnp.zeros(awp.shape[1:], F32)
    coefs[0].wait()
    expand(bv, bx, tokens, n_state)
    coefs[1].wait()
    expand(cv, cx, tokens, n_state)
    coefs[2].wait()
    for k in range(3):
        load(k, 3 + k, 0, 2 * TILES).wait()
    own_tile, own_row = chip // share, lax.rem(chip, share) * r
    for q in range(pieces):
        mine[q] = av[:, lanes_of(2 * q + core, own_tile)] * (-LOG2E)
        for i in range(r):
            own[q, i : i + 1] = mine.at[q][pl.ds(own_row + i, SUB, stride=0), :][:1]

    def gather(u):
        q, odd = u // 2, lax.rem(u, 2)

        @pl.when(u == 2)
        def _():
            for k in range(3):
                load(k, 6 + k, 0, blocks * (TILES - 1)).wait()

        summarize(q, lax.rem(1 - core + odd, 2))

        @pl.when(u == 0)
        def _():
            pl.semaphore_wait(barrier, n // pace - 1 + (pace == 2))

        @pl.when(odd == 0)
        def _():
            mate1(q).start()

            @pl.when(q >= 2)
            def _():
                scan(q - 2)

        @pl.when(odd == 1)
        def _():
            merge(q)

    loop(0, 2 * pieces, gather)
    split(0)

    def turn(u):
        q, odd = u // 2, lax.rem(u, 2)
        return q, odd, lax.rem(core + odd + (q + pieces - 1) // pieces, 2)

    def finish(u):
        q, odd, half = turn(u)
        forward(q, half, 0)
        backward(q, half, 0, True, True)

        @pl.when(u == 0)
        def _():
            scan(pieces - 2)
            mate2(0).wait_recv()

        @pl.when(u == 1)
        def _():
            scan(pieces - 1)
            mate3(0).start()

        @pl.when((1 - odd) * q >= 1)
        def _():
            mate3(q).start()

        @pl.when(u == 2)
        def _():
            spread(0)

        @pl.when(odd * q >= 1)
        def _():
            spread(q)

        @pl.when(odd == 0)
        def _():
            split(q + 1)

        @pl.when(odd == 1)
        def _():
            mate2(q + 1).wait_recv()

    def chain(u):
        q, odd, half = turn(u)
        forward(q, half, odd)
        backward(q, half, odd, True, False)

        @pl.when(odd == 0)
        def _():
            mate3(q).start()

        @pl.when(odd == 1)
        def _():
            spread(q)

    def sums(u):
        q, odd, half = turn(u)
        backward(q, half, odd, False, True)

    loop(0, 2 * pieces - 2, finish)
    loop(2 * pieces - 2, 2 * pieces, chain)
    loop(2 * pieces - 2, 2 * pieces, sums)

    my_tile = me // per
    my_row = my_tile // blocks
    my_half = lax.rem(lax.rem(my_tile, blocks) + 2 * blocks - 2 * my_row, 2)

    def landed(c):
        sender = 2 * c + my_half

        @pl.when(sender != me)
        def _():
            remote(out3.at[0], in3.at[c], i3s.at[0], i3r.at[c], mate).wait_recv()

    loop(0, chips, landed)
    gr_ref[...] = lax.fori_loop(
        0, chips, lambda c, total: total + in3[c], jnp.zeros((n_state, width), F32)
    )
    for q in range(pieces):
        for copy in (mate1(q), mate2(q), mate3(q)):
            copy.wait_send()
        chip_all(out1, in1, i1s, i1r, q).wait_send()
        chip_all(out2, in2, i2s, i2r, q).wait_send()
        for jj in range(TILES):
            for s in range(per):
                slot, dest = (q * TILES + jj) * per + s, owner(q, jj, s)

                @pl.when(dest != me)
                def _():
                    rate_copy(slot, dest).wait_send()


def hand_out(
    giv, gsv, accb, accc, gr_ref, gi_hbm, gs_hbm, gb_hbm, gc_hbm, gr_hbm, gb_ref, gc_ref, sems
):
    tokens, n_state = accb.shape[:2]
    pairs = [(giv, gi_hbm), (gsv, gs_hbm), (gr_ref, gr_hbm), (gb_ref, gb_hbm), (gc_ref, gc_hbm)]
    copies = [pltpu.make_async_copy(src, dst, sems.at[k]) for k, (src, dst) in enumerate(pairs)]
    for copy in copies[:3]:
        copy.start()
    lane_sums(accb, gb_ref, tokens, n_state)
    copies[3].start()
    lane_sums(accc, gc_ref, tokens, n_state)
    copies[4].start()
    for copy in copies:
        copy.wait()


def shards(n, inputs, step_sizes, cotangent, input_coeffs, output_coeffs, decay_rates):
    n_state, channels = decay_rates.shape
    tokens = inputs.shape[0]
    width = channels // n
    per = LANES // width
    chips = n // 2
    block = TILES * LANES
    blocks = channels // block
    pieces = blocks // 2
    r = n_state * TILES // chips
    assert r * chips == n_state * TILES and per * width == LANES
    wide = pltpu.VMEM((tokens, n_state, LANES), F32)
    rows = pltpu.VMEM((blocks, TILES, tokens + SUB, LANES), F32)
    part = pltpu.VMEM((TILES, tokens, LANES), F32)
    fold = pltpu.VMEM((2, TILES, (GROUP + 1) * SUB, LANES), F32)
    full = pltpu.VMEM((tokens, channels), jnp.bfloat16)
    small = pltpu.VMEM((n_state, tokens), F32)
    hbm = pl.BlockSpec(memory_space=pl.ANY)
    vmem = pl.BlockSpec(memory_space=pltpu.VMEM)
    sems = pltpu.SemaphoreType.DMA((pieces,))
    outs = [
        jax.ShapeDtypeStruct((tokens, channels), jnp.bfloat16),
        jax.ShapeDtypeStruct((tokens, channels), jnp.bfloat16),
        jax.ShapeDtypeStruct((n_state, tokens), F32),
        jax.ShapeDtypeStruct((n_state, tokens), F32),
        jax.ShapeDtypeStruct((n_state, width), F32),
    ]
    held = [pltpu.VMEM(o.shape, o.dtype) for o in outs]
    held[2:4] = [wide, wide]
    results = pl.pallas_call(
        partial(whole_kernel, n),
        name="whole",
        in_specs=[hbm] * 6,
        out_specs=[vmem] * 5,
        out_shape=held,
        scratch_shapes=[
            full, full, full, small, small, pltpu.VMEM((n_state, channels), F32),
            wide, wide, rows, rows, rows,
            pltpu.VMEM((blocks, tokens, TILES, n_state, LANES), F32),
            pltpu.VMEM((2, tokens, TILES, n_state, LANES), F32),
            fold, fold, part, part,
            pltpu.VMEM((pieces, n_state, LANES), F32),
            pltpu.VMEM((pieces, r, LANES), F32),
            pltpu.VMEM((pieces, 2, 2 * n_state + 1, block), F32),
            pltpu.VMEM((pieces, 2 * n_state + 1, block), F32),
            pltpu.VMEM((pieces, chips, 2 * r + 1, LANES), F32),
            pltpu.VMEM((pieces, chips, 2 * r + 1, LANES), F32),
            pltpu.VMEM((pieces, chips, 2 * r, LANES), F32),
            pltpu.VMEM((pieces, chips, 2 * r, LANES), F32),
            pltpu.VMEM((2 * n_state, block), F32),
            pltpu.VMEM((pieces, 2 * n_state, block), F32),
            pltpu.VMEM((pieces, 2, 2 * n_state, block), F32),
            pltpu.VMEM((pieces, 2, n_state, block), F32),
            pltpu.VMEM((pieces, n_state, block), F32),
            pltpu.VMEM((pieces * TILES * per, n_state, width), F32),
            pltpu.VMEM((chips, n_state, width), F32),
            pltpu.SemaphoreType.DMA((9,)),
            sems, sems, sems, sems, sems, sems, sems, sems, sems, sems,
            pltpu.SemaphoreType.DMA((pieces * TILES * per,)),
            pltpu.SemaphoreType.DMA((chips,)),
        ],
        compiler_params=pltpu.CompilerParams(
            collective_id=0, has_side_effects=True, vmem_limit_bytes=58 * 1024 * 1024
        ),
    )(inputs, step_sizes, cotangent, input_coeffs, output_coeffs, decay_rates)
    return pl.pallas_call(
        hand_out,
        name="hand_out",
        in_specs=[vmem] * 5,
        out_specs=[hbm] * 5,
        out_shape=outs,
        scratch_shapes=[small, small, pltpu.SemaphoreType.DMA((5,))],
        compiler_params=pltpu.CompilerParams(vmem_limit_bytes=8 * 1024 * 1024),
    )(*[pltpu.with_memory_space_constraint(x, pltpu.VMEM) for x in results])


def solution(mesh):
    placed = (P("seq", None), P("seq", None), P("seq", None), P(None, "seq"), P(None, "seq"), P())
    return jax.shard_map(
        partial(shards, mesh.shape["seq"]),
        mesh=mesh,
        in_specs=placed,
        out_specs=(P("seq", None), P("seq", None), P(None, "seq"), P(None, "seq"), P(None, "seq")),
        check_vma=False,
    )
```
